128 devices in a mesh: lat: 8 (over z, core), lon: 16 (over x, y).
Axes of the slice: x: 4, y: 4, z: 4, core: 2. Of those that a mesh axis runs over, the one named last changes fastest.
Arguments:
- observations: bfloat16 [196608, 128], P(('lat', 'lon')), may hold values from -6 to 6
- owner_device: int32 [196608, 1], P(('lat', 'lon')), may hold values from 0 to 127; in each aligned block of 1536 rows (0 to 1535, 1536 to 3071, ...) at most 24 rows name the same one
- local_cell: int32 [196608], P(('lat', 'lon')), may hold values from 0 to 383
- valid_counts: int32 [128], P(('lat', 'lon')), may hold values from 768 to 1536
- weight_in: bfloat16 [128, 256], replicated, may hold values from -0.5 to 0.5
- bias_in: float32 [256], replicated, may hold values from -3 to 3
- weight_out: bfloat16 [256, 256], replicated, may hold values from -0.375 to 0.375
- kernel_taps: float32 [9, 256], replicated, may hold values from -2 to 2
- cotangent: bfloat16 [128, 384, 256], P(('lat', 'lon')), may hold values from -6 to 6
Outputs:
- grid_out: bfloat16 [128, 384, 256], P(('lat', 'lon'))
- grad_weight_in: float32 [128, 256], replicated
- grad_bias_in: float32 [256], replicated
- grad_weight_out: float32 [256, 256], replicated
- grad_kernel: float32 [9, 256], replicated
The draws below stay inside these ranges and needn't reach their ends.
Inputs may be any that keep to these rules, and one draw needn't show every extreme that they name: `owner_device`: within the rows of one block, at most 24 rows name one owner, and in every draw some block names some owner exactly 24 times.
All inputs are finite; a program needn't handle non-finite values.
Results may differ from the reference program's by a relative error of at most 0.0065.
Values may be sent and summed in bfloat16 or wider, within the bound.
A program may use at most 64 MiB of HBM per device.

```python
import math
import jax
import jax.numpy as jnp
import numpy as np
from jax import lax

FEAT = 128
HIDDEN_SIZE = 256
CHANNELS = 256
TAPS = 9
TLAT = 16
TLON = 24
OBS_DEV = 1536
GLAT = 128
GLON = 384
OBS_ALL = 196608
CAP = 24
N_LAT = 8
N_LON = 16


def with_ends(result, rng, low, high):
    extent = result.shape
    spot = [jax.random.randint(jax.random.fold_in(rng, axis), (), 0, extent[axis]) for axis in range(len(extent))]
    result = result.at[tuple(spot)].set(low)
    longest = extent.index(max(extent))
    spot[longest] = (spot[longest] + 1) % extent[longest]
    return result.at[tuple(spot)].set(high)


def levels(rng, shape, shards, least, top_value):
    factor_of, own = 1.0, jax.random.fold_in(rng, 6)
    for axis_at, parts in shards:
        heights = jnp.exp(jax.random.uniform(jax.random.fold_in(own, axis_at), (parts,), jnp.float32, least / len(shards), top_value / len(shards)))
        factor_of = factor_of * jnp.repeat(heights, shape[axis_at] // parts).reshape([-1 if axis == axis_at else 1 for axis in range(len(shape))])
    return factor_of


def deal_out(stream_key, own, number, rows, count, top, reach, slope):
    sequence = jax.random.permutation(stream_key, count)
    packed, ordinary = portions_of(count, rows * top, reach, slope, True), portions_of(count, rows * top, reach, slope, False)
    places = jnp.arange(count)

    def named(sizes, turn):
        used = int((sizes > 0).sum())
        fixed = max(1, used // 4)
        shifted = fixed + (places - fixed + turn * (used - fixed)) % max(1, count - fixed)
        return jnp.zeros((count,), jnp.int32).at[sequence[jnp.where(places < fixed, places, shifted)]].set(jnp.asarray(sizes, jnp.int32))

    sizes = jnp.where(number % 4 == 0, named(packed, number // 4), named(ordinary, number - number // 4 - 1))
    mixed = jax.random.permutation(jax.random.fold_in(own, 3), count)
    source_of, taker = mixed[0:count // 2 * 2:2], mixed[1:count // 2 * 2:2]
    room = jnp.minimum(sizes[source_of] - 1, reach - sizes[taker]) // 2
    room = jnp.where((source_of == sequence[0]) | (taker == sequence[0]) | (sizes[taker] == 0), 0, jnp.maximum(room, 0))
    shifted = jax.random.randint(jax.random.fold_in(own, 4), (count // 2,), 0, 1 << 20) % (room + 1)
    sizes = sizes.at[source_of].add(-shifted).at[taker].add(shifted)
    items = jnp.searchsorted(jnp.cumsum(sizes), jnp.arange(rows * top), side="right").astype(jnp.int32)
    grid = items.reshape(top, rows).T
    grid = grid[jax.random.permutation(jax.random.fold_in(own, 1), rows)]
    turn = jax.random.randint(jax.random.fold_in(own, 2), (rows, 1), 0, top)
    return jnp.take_along_axis(grid, (jnp.arange(top)[None, :] + turn) % top, axis=1)


def portions_of(amount, total, limit, lean, full):
    weights = [(1 << 20) // math.isqrt(standing ** lean) + 1 for standing in range(1, amount + 1)]
    largest = limit if full else min(limit, max(-(-total // amount), total * weights[0] // sum(weights)))
    least = 1 if total - largest >= amount - 1 else 0
    counts, surplus = [largest] + [least] * (amount - 1), total - largest - least * (amount - 1)
    while surplus > 0:
        movable = [i for i in range(1, amount) if counts[i] < largest] or [i for i in range(1, amount) if counts[i] < limit]
        whole, left = sum([weights[i] for i in movable]), surplus
        for i in movable:
            extra = min(limit - counts[i], max(1, left * weights[i] // whole), surplus)
            counts[i] = counts[i] + extra
            surplus = surplus - extra
    return np.array(counts)


def bell_draw(own_key, shape, width, bound, split=(), kind=jnp.bfloat16):
    array = width * jax.random.normal(own_key, shape, jnp.float32)
    if split:
        array = array * levels(own_key, shape, split, -0.22, 0.18)
    return jnp.clip(array, -bound, bound).astype(kind)


def setup_inputs(seed: int = 0) -> dict:
    splits = jax.random.split(jax.random.key(seed), 10)
    observations = bell_draw(splits[0], (OBS_ALL, FEAT), 1.0, 6.0, ((0, 128),))
    owner_device_keys = jax.random.split(jax.random.fold_in(splits[1], 1), OBS_ALL // OBS_DEV)
    owner_device_turns = jax.random.permutation(jax.random.fold_in(splits[1], 3), OBS_ALL // OBS_DEV)
    owner_device = jax.vmap(lambda own, number: deal_out(jax.random.fold_in(splits[1], 2), own, number, OBS_DEV, N_LAT * N_LON, 1, CAP, 2))(owner_device_keys, owner_device_turns).reshape((OBS_ALL, 1))
    local_cell = with_ends(jax.random.randint(splits[2], (OBS_ALL,), 0, TLAT * TLON), jax.random.fold_in(splits[2], 1), 0, (TLAT * TLON) - 1).astype(jnp.int32)
    valid_counts = with_ends(jax.random.randint(splits[3], (N_LAT * N_LON,), OBS_DEV // 2, OBS_DEV + 1), jax.random.fold_in(splits[3], 1), OBS_DEV // 2, OBS_DEV).astype(jnp.int32)
    weight_in = bell_draw(splits[4], (FEAT, HIDDEN_SIZE), FEAT ** -0.5, 0.5)
    bias_in = bell_draw(splits[5], (HIDDEN_SIZE,), 0.5, 3.0, (), jnp.float32)
    weight_out = bell_draw(splits[6], (HIDDEN_SIZE, CHANNELS), HIDDEN_SIZE ** -0.5, 0.375)
    kernel_taps = bell_draw(splits[7], (TAPS, CHANNELS), 0.33, 2.0, (), jnp.float32)
    cotangent = bell_draw(splits[8], (GLAT, GLON, CHANNELS), 1.0, 6.0, ((0, 128),))
    return {"observations": observations, "owner_device": owner_device, "local_cell": local_cell, "valid_counts": valid_counts, "weight_in": weight_in, "bias_in": bias_in, "weight_out": weight_out, "kernel_taps": kernel_taps, "cotangent": cotangent}


OFFSETS = [(shift_lat, shift_lon) for shift_lat in (-1, 0, 1) for shift_lon in (-1, 0, 1)]

def pad_grid(values):
    wrapped = jnp.concatenate([values[:, -1:], values, values[:, :1]], axis=1)
    return jnp.pad(wrapped, ((1, 1), (0, 0), (0, 0)))

def encoder(rows, weight_in, bias_in, weight_out):
    before = jnp.dot(rows, weight_in, preferred_element_type=jnp.float32) + bias_in
    hidden = jax.nn.gelu(before).astype(jnp.bfloat16)
    encoded = jnp.dot(hidden, weight_out, preferred_element_type=jnp.float32).astype(jnp.bfloat16)
    return (before, hidden, encoded)

def local_grads(rows, before, hidden, upstream, weight_out):
    contract = (((0,), (0,)), ((), ()))
    grad_out = lax.dot_general(hidden, upstream, contract, preferred_element_type=jnp.float32)
    back = lax.dot_general(upstream, weight_out, (((1,), (1,)), ((), ())), preferred_element_type=jnp.float32)
    _, pullback = jax.vjp(jax.nn.gelu, before)
    pre_grad = pullback(back)[0].astype(jnp.bfloat16)
    grad_in = lax.dot_general(rows, pre_grad, contract, preferred_element_type=jnp.float32)
    grad_bias = lax.optimization_barrier(jnp.sum(pre_grad.astype(jnp.float32), axis=0))
    return (grad_in, grad_bias, grad_out)

def reference(observations, owner_device, local_cell, valid_counts, weight_in, bias_in, weight_out, kernel_taps, cotangent):
    devices_all = N_LAT * N_LON
    cells_total = GLAT * GLON
    row_blocks = observations.reshape(devices_all, OBS_DEV, FEAT)
    owner_blocks = owner_device.reshape(devices_all, OBS_DEV)
    local_blocks = local_cell.reshape(devices_all, OBS_DEV)

    def destination(owner_row, local_row, count):
        valid_rows = jnp.arange(OBS_DEV, dtype=jnp.int32) < count
        lat_cell = owner_row // N_LON * TLAT + local_row // TLON
        lon_cell = owner_row % N_LON * TLON + local_row % TLON
        return jnp.where(valid_rows, lat_cell * GLON + lon_cell, cells_total).astype(jnp.int32)

    def forward_step(deposit, item):
        rows, owner_row, local_row, count = item
        target = destination(owner_row, local_row, count)
        _, _, encoded = encoder(rows, weight_in, bias_in, weight_out)
        deposit = deposit + jax.ops.segment_sum(encoded.astype(jnp.float32), target, num_segments=cells_total + 1)
        return (deposit, None)
    deposit, _ = lax.scan(forward_step, jnp.zeros((cells_total + 1, CHANNELS), jnp.float32), (row_blocks, owner_blocks, local_blocks, valid_counts))
    point = deposit[:cells_total].reshape(GLAT, GLON, CHANNELS)
    padded = pad_grid(point)
    grid_field = jnp.zeros((GLAT, GLON, CHANNELS), jnp.float32)
    for tap_index, (shift_lat, shift_lon) in enumerate(OFFSETS):
        window = padded[1 + shift_lat:1 + shift_lat + GLAT, 1 + shift_lon:1 + shift_lon + GLON]
        grid_field = grid_field + kernel_taps[tap_index] * window
    grid_out = grid_field.astype(jnp.bfloat16)
    loss_scale = 1.0 / math.sqrt(OBS_DEV * devices_all)
    cot_float = cotangent.astype(jnp.float32)
    cot_padded = pad_grid(cot_float)
    kernel_rows = []
    adjoint = jnp.zeros((GLAT, GLON, CHANNELS), jnp.float32)
    for tap_index, (shift_lat, shift_lon) in enumerate(OFFSETS):
        window = padded[1 + shift_lat:1 + shift_lat + GLAT, 1 + shift_lon:1 + shift_lon + GLON]
        kernel_rows.append(loss_scale * lax.optimization_barrier(jnp.sum(cot_float * window, axis=(0, 1))))
        back_window = cot_padded[1 - shift_lat:1 - shift_lat + GLAT, 1 - shift_lon:1 - shift_lon + GLON]
        adjoint = adjoint + kernel_taps[tap_index] * back_window
    grad_kernel = jnp.stack(kernel_rows)
    adjoint = (loss_scale * adjoint).astype(jnp.bfloat16)
    adjoint_rows = jnp.concatenate([adjoint.reshape(cells_total, CHANNELS), jnp.zeros((1, CHANNELS), jnp.bfloat16)], axis=0)

    def backward_step(totals, item):
        rows, owner_row, local_row, count = item
        target = destination(owner_row, local_row, count)
        before, hidden, _ = encoder(rows, weight_in, bias_in, weight_out)
        upstream = adjoint_rows[target]
        grads = local_grads(rows, before, hidden, upstream, weight_out)
        return (tuple((total + grad for total, grad in zip(totals, grads))), None)
    zeros_start = (jnp.zeros((FEAT, HIDDEN_SIZE), jnp.float32), jnp.zeros((HIDDEN_SIZE,), jnp.float32), jnp.zeros((HIDDEN_SIZE, CHANNELS), jnp.float32))
    totals, _ = lax.scan(backward_step, zeros_start, (row_blocks, owner_blocks, local_blocks, valid_counts))
    return (grid_out, totals[0], totals[1], totals[2], grad_kernel)
```

```python
import functools
import math

import jax
import jax.numpy as jnp
from jax import lax
from jax.experimental import pallas as pl
from jax.experimental.pallas import tpu as pltpu
from jax.sharding import PartitionSpec as P

MESH = pl.DeviceIdType.MESH
F32, BF16, I32 = jnp.float32, jnp.bfloat16, jnp.int32
NT = (((1,), (1,)), ((), ()))
TAPS = [(a, b) for a in (-1, 0, 1) for b in (-1, 0, 1)]

N_DEV, N_GRP, GRP = 128, 8, 16
OBS, FEAT, HID, CH = 1536, 128, 256, 256
CAP = 24
SLOTS = GRP * CAP
TLAT, TLON = 16, 24
CELLS = TLAT * TLON
GLON = 384
CHUNKS_IN, CHUNKS_OUT, CHUNKS_SMALL = 32, 64, 3
SCALE = 1.0 / math.sqrt(OBS * N_DEV)
C0, C1 = math.sqrt(2.0 / math.pi), 0.044715


def iota(shape, dim):
    return lax.broadcasted_iota(I32, shape, dim)


def mm(a, b):
    return jnp.dot(a, b, preferred_element_type=F32)


def mm_nt(a, b):
    return lax.dot_general(a, b, NT, preferred_element_type=F32)


def kernel(
    obs_ref, owner_ref, cell_ref, count_ref, w_in_ref, bias_ref, w_out_ref, taps_ref, cot_ref,
    grid_ref, g_in_ref, g_bias_ref, g_out_ref, g_taps_ref,
    send_rows, recv_rows, send_cells, recv_cells, send_cot, recv_cot, cot_f, dep, send_grid,
    chunks, parts, red, shared, acc_in, acc_out, acc_bias, adj_t, sel_rows,
    row_send, row_recv, cell_send, cell_recv, cot_send, cot_recv, fwd_send, fwd_recv,
    part_send, part_recv, share_send, share_recv, halo_send, halo_recv, grid_send, grid_recv,
):
    lat, lon = lax.axis_index("lat"), lax.axis_index("lon")
    z, c, x, y = lax.div(lat, 2), lax.rem(lat, 2), lax.div(lon, 4), lax.rem(lon, 4)
    me = lat * GRP + lon
    lons = [lax.rem(x + j // 4, 4) * 4 + lax.rem(y + j % 4, 4) for j in range(GRP)]

    def lat_of(g):
        return lax.rem(z + lax.div(g, 2), 4) * 2 + lax.rem(c + lax.rem(g, 2), 2)

    def each_peer(fn):
        def body(g, carry):
            to_lat = lat_of(g)
            for j in range(GRP):
                if j:
                    fn(g, j, to_lat, lons[j])
                else:
                    pl.when(g > 0)(lambda: fn(g, 0, to_lat, lons[0]))
            return carry

        lax.fori_loop(0, N_GRP, body, 0)

    def remote(src, dst, send, recv, to_lat, to_lon):
        return pltpu.make_async_remote_copy(
            src_ref=src, dst_ref=dst, send_sem=send, recv_sem=recv,
            device_id=(to_lat, to_lon), device_id_type=MESH,
        )

    def wait_sent(ref, sem):
        remote(ref, ref, sem, sem, lat, lon).wait_send()

    def wait_got(ref, sem):
        remote(ref, ref, sem, sem, lat, lon).wait_recv()

    dep[...] = jnp.zeros_like(dep)
    recv_cot[0] = jnp.zeros(recv_cot.shape[1:], BF16)
    recv_cot[TLAT + 1] = jnp.zeros(recv_cot.shape[1:], BF16)

    barrier = pltpu.get_barrier_semaphore()

    def greet(g, j, to_lat, to_lon):
        pl.semaphore_signal(barrier, inc=1, device_id=(to_lat, to_lon), device_id_type=MESH)

    each_peer(greet)

    owner = owner_ref[...]
    valid = iota((1, OBS), 1) < count_ref[0]
    o_lat, o_lon = owner // GRP, owner % GRP
    rel = (
        (((o_lat // 2) - z + 4) % 4) * 32
        + ((o_lat % 2) - c + 2) % 2 * 16
        + ((o_lon // 4) - x + 4) % 4 * 4
        + ((o_lon % 4) - y + 4) % 4
    )
    rel = jnp.where(valid, rel, -1)
    upto = jnp.where(iota((256, 256), 0) <= iota((256, 256), 1), 1.0, 0.0).astype(BF16)
    peer_ids = iota((N_DEV, 256), 0)
    carry = jnp.zeros((N_DEV, 1), F32)
    ranks = []
    for i in range(OBS // 256):
        hit = jnp.where(peer_ids == rel[:, i * 256 : (i + 1) * 256], 1.0, 0.0)
        count = mm(hit.astype(BF16), upto) + carry
        ranks.append(jnp.sum(hit * count, axis=0, keepdims=True) - 1.0)
        carry = count[:, 255:256]
    rank = jnp.concatenate(ranks, axis=1).astype(I32)
    key = jnp.where(valid, rel * CAP + rank, -1)

    value = cell_ref[...] + 1
    high = jnp.where(value >= 256, 1.0, 0.0)
    low = value.astype(F32) - 256.0 * high
    cells_high = jnp.zeros((N_DEV, 128), F32)
    cells_low = jnp.zeros((N_DEV, 128), F32)
    for i in range(OBS // 256):
        part = slice(i * 256, (i + 1) * 256)
        hit = jnp.where(peer_ids == rel[:, part], 1.0, 0.0)
        place = jnp.where(iota((128, 256), 0) == rank[:, part], 1.0, 0.0).astype(BF16)
        cells_high += mm_nt((hit * high[:, part]).astype(BF16), place)
        cells_low += mm_nt((hit * low[:, part]).astype(BF16), place)
    cells = (256.0 * cells_high + cells_low).reshape(N_GRP, GRP, 128)
    send_cells[...] = cells
    recv_cells[0, 0:1] = cells[0, 0:1]

    pl.semaphore_wait(barrier, N_DEV - 1)

    def send_cell(g, j, to_lat, to_lon):
        remote(
            send_cells.at[g, pl.ds(j, 1)], recv_cells.at[g, pl.ds(j, 1)],
            cell_send.at[g], cell_recv.at[g], to_lat, to_lon,
        ).start()

    each_peer(send_cell)

    def pack(g, carry):
        total = jnp.zeros((SLOTS, FEAT), F32)
        for i in range(OBS // 256):
            part = slice(i * 256, (i + 1) * 256)
            take = jnp.where(iota((SLOTS, 256), 0) + g * SLOTS == key[:, part], 1.0, 0.0)
            total += mm(take.astype(BF16), obs_ref[part, :])
        send_rows[pl.ds(g * GRP, GRP)] = total.reshape(GRP, CAP, FEAT).astype(BF16)
        to_lat = lat_of(g)
        for j in range(GRP):
            def send_row(j=j):
                remote(
                    send_rows.at[g * GRP + j], recv_rows.at[g * GRP + j],
                    row_send.at[g], row_recv.at[g], to_lat, lons[j],
                ).start()

            if j:
                send_row()
            else:
                pl.when(g > 0)(send_row)
        return carry

    lax.fori_loop(0, N_GRP, pack, 0)
    recv_rows[0] = send_rows[0]

    where_from = iota((GRP * 32, GLON), 0)
    tile, slot = where_from // 32, where_from % 32
    column = jnp.where(
        slot < TLON,
        tile * TLON + slot,
        jnp.where(
            slot == TLON,
            (tile * TLON + GLON - 1) % GLON,
            jnp.where(slot == TLON + 1, (tile * TLON + TLON) % GLON, -1),
        ),
    )
    pick = jnp.where(column == iota((GRP * 32, GLON), 1), 1.0, 0.0).astype(BF16)
    send_cot[...] = mm(pick, cot_ref[...]).reshape(GRP, 32, CH).astype(BF16)
    for j in range(1, GRP):
        remote(
            send_cot.at[lons[j]], recv_cot.at[1 + lon], cot_send, cot_recv, lat, lons[j]
        ).start()
    recv_cot[1 + lon] = send_cot[lon]

    w_in_t = w_in_ref[...].astype(F32).T.astype(BF16)
    w_out = w_out_ref[...]
    w_out_t = w_out.astype(F32).T.astype(BF16)
    bias_t = jnp.broadcast_to(bias_ref[...], (128, HID)).T[:, 0:1]
    for g in range(N_GRP):
        got = recv_cells.at[g] if g else recv_cells.at[0, pl.ds(0, GRP - 1)]
        wait_got(got, cell_recv.at[g])
    codes = recv_cells[...].reshape(N_DEV, 128)
    high = jnp.where(codes >= 256.0, 1.0, 0.0)
    spread = jnp.where(iota((128, SLOTS), 0) == iota((128, SLOTS), 1) % CAP, 1.0, 0.0).astype(BF16)
    codes = 256.0 * mm(high.astype(BF16), spread) + mm((codes - 256.0 * high).astype(BF16), spread)
    own = iota((GRP, SLOTS), 0) == iota((GRP, SLOTS), 1) // CAP
    for g in range(N_GRP):
        mine = jnp.where(own, codes[g * GRP : (g + 1) * GRP], 0.0)
        sel_rows[g] = jnp.sum(mine, axis=0, keepdims=True).astype(I32) - 1

    wait_got(recv_cot.at[pl.ds(0, GRP - 1)], cot_recv)

    @pl.when(lat > 0)
    def _():
        remote(
            recv_cot.at[1], recv_cot.at[TLAT + 1], fwd_send.at[0], fwd_recv.at[0], lat - 1, lon
        ).start()

    @pl.when(lat < N_GRP - 1)
    def _():
        remote(
            recv_cot.at[TLAT], recv_cot.at[0], fwd_send.at[1], fwd_recv.at[1], lat + 1, lon
        ).start()

    @pl.when(lat < N_GRP - 1)
    def _():
        wait_got(recv_cot.at[TLAT + 1], fwd_recv.at[0])

    @pl.when(lat > 0)
    def _():
        wait_got(recv_cot.at[0], fwd_recv.at[1])

    cot_all = recv_cot[...].astype(F32)
    cot_f[:, 8:32, :] = cot_all[:, 0:TLON]
    cot_f[:, 7:8, :] = cot_all[:, TLON : TLON + 1]
    cot_f[:, 32:33, :] = cot_all[:, TLON + 1 : TLON + 2]

    def adjoint_row(r, carry):
        total = jnp.zeros((TLON, CH), F32)
        for k, (a, b) in enumerate(TAPS):
            total += taps_ref[k : k + 1, :] * cot_f[r + 1 - a, 8 - b : 8 - b + TLON, :]
        send_grid[r] = (SCALE * total).astype(BF16)
        return carry

    lax.fori_loop(0, TLAT, adjoint_row, 0)
    adj_t[...] = send_grid[...].astype(F32).reshape(CELLS, CH).T.astype(BF16)

    acc_in[...] = jnp.zeros_like(acc_in)
    acc_out[...] = jnp.zeros_like(acc_out)
    acc_bias[...] = jnp.zeros_like(acc_bias)

    def work(g):
        rows = recv_rows[pl.ds(g * GRP, GRP)].astype(F32).reshape(SLOTS, FEAT).astype(BF16)
        before = mm_nt(w_in_t, rows) + bias_t
        square = before * before
        t = jnp.tanh(C0 * before * (1.0 + C1 * square))
        half = 0.5 * (1.0 + t)
        slope = half + 0.5 * before * (1.0 - t * t) * (C0 * (1.0 + 3.0 * C1 * square))
        hidden = (before * half).astype(BF16)
        encoded = mm(w_out_t, hidden).astype(BF16)
        place = jnp.where(iota((CELLS, SLOTS), 0) == sel_rows[g], 1.0, 0.0).astype(BF16)
        add = mm_nt(place, encoded).reshape(TLAT, TLON, CH)
        dep[1 : 1 + TLAT, 8 : 8 + TLON, :] += add
        up = mm(adj_t[...], place).astype(BF16)
        pre = (mm(w_out, up) * slope).astype(BF16)
        acc_out[...] += mm_nt(hidden, up)
        acc_in[...] += mm(pre, rows)
        pre = pre.astype(F32)
        acc_bias[...] += pre[:, 0:128] + pre[:, 128:256] + pre[:, 256:384]

    for g in range(N_GRP):
        got = recv_rows.at[pl.ds(g * GRP, GRP if g else GRP - 1)]
        wait_got(got, row_recv.at[g])
        work(g)

    north, south = lat > 0, lat < N_GRP - 1
    west, east = lax.rem(lon + 15, GRP), lax.rem(lon + 1, GRP)
    core = (1, TLAT)
    first, last = (1, 1), (TLAT, 1)
    above, below = (0, 1), (TLAT + 1, 1)
    wide, left, right = (8, TLON), (8, 1), (8 + TLON - 1, 1)
    before_left, after_right = (7, 1), (8 + TLON, 1)
    halos = [
        (None, lat, west, core, left, core, after_right),
        (None, lat, east, core, right, core, before_left),
        (north, lat - 1, lon, first, wide, below, wide),
        (south, lat + 1, lon, last, wide, above, wide),
        (north, lat - 1, west, first, left, below, after_right),
        (north, lat - 1, east, first, right, below, before_left),
        (south, lat + 1, west, last, left, above, after_right),
        (south, lat + 1, east, last, right, above, before_left),
    ]
    comes = [None, None, south, north, south, south, north, north]

    def at(rows, columns):
        return dep.at[pl.ds(*rows), pl.ds(*columns), :]

    for i, (there, to_lat, to_lon, sr, sc, dr, dc) in enumerate(halos):
        def send_halo(i=i, to_lat=to_lat, to_lon=to_lon, sr=sr, sc=sc, dr=dr, dc=dc):
            remote(
                at(sr, sc), at(dr, dc), halo_send.at[i], halo_recv.at[i], to_lat, to_lon
            ).start()

        send_halo() if there is None else pl.when(there)(send_halo)

    def taps_row(r, totals):
        mine = dep[r + 1, 8 : 8 + TLON, :]
        return tuple(
            total + mine * cot_f[r + 1 - a, 8 - b : 8 - b + TLON, :]
            for total, (a, b) in zip(totals, TAPS)
        )

    totals = lax.fori_loop(0, TLAT, taps_row, (jnp.zeros((TLON, CH), F32),) * 9)
    small = [SCALE * jnp.sum(t, axis=0, keepdims=True) for t in totals]
    small.append(jnp.sum(acc_bias[...].T, axis=0, keepdims=True))
    small = [h for s in small for h in (s[:, :128], s[:, 128:])]
    small = jnp.concatenate(small + [jnp.zeros((4, 128), F32)], axis=0)
    small_high = small.astype(BF16)
    small_low = (small - small_high.astype(F32)).astype(BF16)
    chunks[0:32] = acc_in[...].reshape(32, 8, 128).astype(BF16)
    chunks[32:64] = acc_out[:, :128].reshape(32, 8, 128).astype(BF16)
    chunks[64:96] = acc_out[:, 128:].reshape(32, 8, 128).astype(BF16)
    chunks[96:99] = small_high.astype(F32).reshape(3, 8, 128).astype(BF16)
    chunks[99:102] = small_low.astype(F32).reshape(3, 8, 128).astype(BF16)
    chunks[102:128] = jnp.zeros((26, 8, 128), BF16)

    def send_part(g, j, to_lat, to_lon):
        remote(
            chunks.at[to_lat * GRP + to_lon], parts.at[g * GRP + j],
            part_send.at[g], part_recv.at[g], to_lat, to_lon,
        ).start()

    each_peer(send_part)
    parts[0] = chunks[me]

    for i, there in enumerate(comes):
        _, _, _, _, _, dr, dc = halos[i]
        def got_halo(i=i, dr=dr, dc=dc):
            wait_got(at(dr, dc), halo_recv.at[i])

        got_halo() if there is None else pl.when(there)(got_halo)

    def grid_row(r, carry):
        total = jnp.zeros((TLON, CH), F32)
        for k, (a, b) in enumerate(TAPS):
            total += taps_ref[k : k + 1, :] * dep[r + 1 + a, 8 + b : 8 + b + TLON, :]
        send_grid[r] = total.astype(BF16)
        return carry

    lax.fori_loop(0, TLAT, grid_row, 0)
    for j in range(1, GRP):
        remote(
            send_grid.at[lons[j]], grid_ref.at[lon], grid_send, grid_recv, lat, lons[j]
        ).start()
    grid_ref[lon] = send_grid[lon]

    for g in range(N_GRP):
        wait_got(parts.at[pl.ds(g * GRP, GRP if g else GRP - 1)], part_recv.at[g])
    mine = jnp.sum(parts[...].astype(F32), axis=0).astype(BF16)
    red[...] = mine
    shared[me] = mine

    def send_share(g, j, to_lat, to_lon):
        remote(
            red, shared.at[me], share_send.at[g], share_recv.at[g], to_lat, to_lon
        ).start()

    each_peer(send_share)

    for g in range(N_GRP):
        wait_got(shared.at[pl.ds(g * GRP, GRP if g else GRP - 1)], share_recv.at[g])
    whole = shared[...].astype(F32)
    g_in_ref[...] = whole[0:32].reshape(HID, FEAT).T
    g_out_ref[:, :128] = whole[32:64].reshape(HID, 128)
    g_out_ref[:, 128:] = whole[64:96].reshape(HID, 128)
    small = (whole[96:99] + whole[99:102]).reshape(24, 128)
    for k in range(9):
        g_taps_ref[k : k + 1, :128] = small[2 * k : 2 * k + 1]
        g_taps_ref[k : k + 1, 128:] = small[2 * k + 1 : 2 * k + 2]
    g_bias_ref[:, :128] = small[18:19]
    g_bias_ref[:, 128:] = small[19:20]

    wait_got(grid_ref.at[pl.ds(0, GRP - 1)], grid_recv)
    for g in range(N_GRP):
        n = GRP if g else GRP - 1
        wait_sent(send_cells.at[g, pl.ds(0, n)], cell_send.at[g])
        wait_sent(send_rows.at[pl.ds(g * GRP, n)], row_send.at[g])
        wait_sent(chunks.at[pl.ds(g * GRP, n)], part_send.at[g])
        wait_sent(shared.at[pl.ds(g * GRP, n)], share_send.at[g])
    wait_sent(send_cot.at[pl.ds(0, GRP - 1)], cot_send)
    wait_sent(send_grid.at[pl.ds(0, GRP - 1)], grid_send)

    @pl.when(lat > 0)
    def _():
        wait_sent(recv_cot.at[1], fwd_send.at[0])

    @pl.when(lat < N_GRP - 1)
    def _():
        wait_sent(recv_cot.at[TLAT], fwd_send.at[1])

    for i, (there, _, _, sr, sc, _, _) in enumerate(halos):
        def sent_halo(i=i, sr=sr, sc=sc):
            wait_sent(at(sr, sc), halo_send.at[i])

        sent_halo() if there is None else pl.when(there)(sent_halo)


def local(obs, owner, cell, count, w_in, bias, w_out, taps, cot):
    vmem = pl.BlockSpec(memory_space=pltpu.VMEM)
    smem = pl.BlockSpec(memory_space=pltpu.SMEM)
    dma = pltpu.SemaphoreType.DMA
    grid, g_in, g_bias, g_out, g_taps = pl.pallas_call(
        kernel,
        name="encode_step",
        out_shape=(
            jax.ShapeDtypeStruct((GRP, TLON, CH), BF16),
            jax.ShapeDtypeStruct((FEAT, HID), F32),
            jax.ShapeDtypeStruct((1, HID), F32),
            jax.ShapeDtypeStruct((HID, CH), F32),
            jax.ShapeDtypeStruct((9, CH), F32),
        ),
        in_specs=[vmem, vmem, vmem, smem, vmem, vmem, vmem, vmem, vmem],
        out_specs=(vmem,) * 5,
        scratch_shapes=[
            pltpu.VMEM((N_DEV, CAP, FEAT), BF16),
            pltpu.VMEM((N_DEV, CAP, FEAT), BF16),
            pltpu.VMEM((N_GRP, GRP, 128), F32),
            pltpu.VMEM((N_GRP, GRP, 128), F32),
            pltpu.VMEM((GRP, 32, CH), BF16),
            pltpu.VMEM((TLAT + 2, 32, CH), BF16),
            pltpu.VMEM((TLAT + 2, 40, CH), F32),
            pltpu.VMEM((TLAT + 2, 40, CH), F32),
            pltpu.VMEM((TLAT, TLON, CH), BF16),
            pltpu.VMEM((N_DEV, 8, 128), BF16),
            pltpu.VMEM((N_DEV, 8, 128), BF16),
            pltpu.VMEM((8, 128), BF16),
            pltpu.VMEM((N_DEV, 8, 128), BF16),
            pltpu.VMEM((HID, FEAT), F32),
            pltpu.VMEM((HID, CH), F32),
            pltpu.VMEM((HID, 128), F32),
            pltpu.VMEM((CH, CELLS), BF16),
            pltpu.VMEM((N_GRP, 1, SLOTS), I32),
            dma((N_GRP,)), dma((N_GRP,)), dma((N_GRP,)), dma((N_GRP,)),
            dma, dma, dma((2,)), dma((2,)),
            dma((N_GRP,)), dma((N_GRP,)), dma((N_GRP,)), dma((N_GRP,)),
            dma((8,)), dma((8,)), dma, dma,
        ],
        compiler_params=pltpu.CompilerParams(
            collective_id=0, has_side_effects=True, vmem_limit_bytes=50 * 1024 * 1024
        ),
        cost_estimate=pl.CostEstimate(
            flops=4_000_000_000, bytes_accessed=2_000_000, transcendentals=800_000
        ),
    )(
        obs, owner.reshape(1, OBS), cell.reshape(1, OBS), count, w_in, bias.reshape(1, HID),
        w_out, taps, cot.reshape(GLON, CH),
    )
    return (grid.reshape(1, GLON, CH), g_in, g_bias.reshape(HID), g_out, g_taps)


def solution(mesh):
    block = P(("lat", "lon"))
    return jax.shard_map(
        local,
        mesh=mesh,
        in_specs=(block, block, block, block, P(), P(), P(), P(), block),
        out_specs=(block, P(), P(), P(), P()),
        check_vma=False,
    )
```

```python
import functools
import math

import jax
import jax.numpy as jnp
from jax import lax
from jax.experimental import pallas as pl
from jax.experimental.pallas import tpu as pltpu
from jax.sharding import PartitionSpec as P

MESH = pl.DeviceIdType.MESH
F32, BF16, I32 = jnp.float32, jnp.bfloat16, jnp.int32
NT = (((1,), (1,)), ((), ()))
TAPS = [(a, b) for a in (-1, 0, 1) for b in (-1, 0, 1)]

N_DEV, N_GRP, GRP = 128, 8, 16
EARLY = 4
STEP = 2
N_STEP = N_GRP // STEP
OBS, FEAT, HID, CH = 1536, 128, 256, 256
CAP = 24
SLOTS = GRP * CAP
TLAT, TLON = 16, 24
CELLS = TLAT * TLON
WIDE = STEP * SLOTS
GLON = 384
CHUNKS_IN, CHUNKS_OUT, CHUNKS_SMALL = 32, 64, 3
SCALE = 1.0 / math.sqrt(OBS * N_DEV)
C0, C1 = math.sqrt(2.0 / math.pi), 0.044715


def iota(shape, dim):
    return lax.broadcasted_iota(I32, shape, dim)


def mm(a, b):
    return jnp.dot(a, b, preferred_element_type=F32)


def mm_nt(a, b):
    return lax.dot_general(a, b, NT, preferred_element_type=F32)


def offset_at(g, j):
    dx, dy = (j // 4 + 1) % 4, (j + 1) % 4
    return (g + 1 - dx - dy) % 4, (g // 4 + 1) % 2, dx, dy


def kernel(
    obs_hbm, owner_hbm, cell_hbm, count_ref, w_in_hbm, bias_hbm, w_out_hbm, taps_hbm, cot_hbm,
    grid_ref, shared,
    obs_ref, owner_ref, cell_ref, w_in_ref, bias_ref, w_out_ref, taps_ref, cot_ref,
    send_rows, recv_rows, send_cells, recv_cells, send_cot, recv_cot, cot_f, cot_s, dep, send_grid,
    chunks, parts, red, acc_in, acc_out, acc_bias, adj_t, places, ups, backs,
    in_sem, own_sem,
    row_send, row_recv, cell_send, cell_recv, cot_send, cot_recv, edge_send, edge_recv,
    part_send, part_recv, share_send, share_recv, halo_send, halo_recv, grid_send, grid_recv,
):
    ins = [
        pltpu.make_async_copy(src, dst, in_sem.at[i])
        for i, (src, dst) in enumerate([
            (owner_hbm, owner_ref), (cell_hbm, cell_ref), (cot_hbm, cot_ref), (obs_hbm, obs_ref),
            (w_in_hbm, w_in_ref), (w_out_hbm, w_out_ref), (bias_hbm, bias_ref), (taps_hbm, taps_ref),
        ])
    ]
    for copy in ins:
        copy.start()

    lat, lon = lax.axis_index("lat"), lax.axis_index("lon")
    z, c, x, y = lax.div(lat, 2), lax.rem(lat, 2), lax.div(lon, 4), lax.rem(lon, 4)
    me = lat * GRP + lon
    up_edge = (lat > 0) & (lon == 0)
    down_edge = (lat < N_GRP - 1) & (lon == GRP - 1)
    zs, cs, xs, ys = ([lax.rem(at + d, n) for d in range(n)] for at, n in ((z, 4), (c, 2), (x, 4), (y, 4)))

    def peer(g, j):
        dz, dc, dx, dy = offset_at(g, j)
        return zs[dz] * 2 + cs[dc], xs[dx] * 4 + ys[dy]

    lons = [peer(0, j)[1] for j in range(GRP)]

    def members(g):
        return GRP if g < N_GRP - 1 else GRP - 1

    def each_peer(fn):
        for g in range(N_GRP):
            for j in range(members(g)):
                fn(g, j, *peer(g, j))

    def remote(src, dst, send, recv, to_lat, to_lon):
        return pltpu.make_async_remote_copy(
            src_ref=src, dst_ref=dst, send_sem=send, recv_sem=recv,
            device_id=(to_lat, to_lon), device_id_type=MESH,
        )

    def wait_sent(ref, sem):
        remote(ref, ref, sem, sem, lat, lon).wait_send()

    def wait_got(ref, sem):
        remote(ref, ref, sem, sem, lat, lon).wait_recv()

    dep[...] = jnp.zeros_like(dep)
    recv_cot[0] = jnp.zeros(recv_cot.shape[1:], BF16)
    recv_cot[TLAT + 1] = jnp.zeros(recv_cot.shape[1:], BF16)

    barrier = pltpu.get_barrier_semaphore()

    def greet(g, j, to_lat, to_lon):
        pl.semaphore_signal(barrier, inc=1, device_id=(to_lat, to_lon), device_id_type=MESH)

    each_peer(greet)

    ins[0].wait()
    ins[1].wait()
    owner = owner_ref[...]
    valid = iota((1, OBS), 1) < count_ref[0]
    o_lat, o_lon = owner // GRP, owner % GRP
    dz, dc = (o_lat // 2 - z + 4) % 4, (o_lat - c + 2) % 2
    dx, dy = (o_lon // 4 - x + 4) % 4, (o_lon - y + 4) % 4
    group = (1 - dc) * 4 + (dz + dx + dy + 3) % 4
    rel = group * GRP + (dx + 3) % 4 * 4 + (dy + 3) % 4
    rel = jnp.where(valid, rel, -1)
    upto = jnp.where(iota((256, 256), 0) <= iota((256, 256), 1), 1.0, 0.0).astype(BF16)
    peer_ids = iota((N_DEV, 256), 0)
    carry = jnp.zeros((N_DEV, 1), F32)
    ranks = []
    for i in range(OBS // 256):
        hit = jnp.where(peer_ids == rel[:, i * 256 : (i + 1) * 256], 1.0, 0.0)
        count = mm(hit.astype(BF16), upto) + carry
        ranks.append(jnp.sum(hit * count, axis=0, keepdims=True) - 1.0)
        carry = count[:, 255:256]
    rank = jnp.concatenate(ranks, axis=1).astype(I32)
    key = jnp.where(valid, rel * CAP + rank, -1)

    value = cell_ref[...].reshape(1, OBS) + 1
    high = jnp.where(value >= 256, 1.0, 0.0)
    low = value.astype(F32) - 256.0 * high
    cells_high = jnp.zeros((N_DEV, 128), F32)
    cells_low = jnp.zeros((N_DEV, 128), F32)
    for i in range(OBS // 256):
        part = slice(i * 256, (i + 1) * 256)
        hit = jnp.where(peer_ids == rel[:, part], 1.0, 0.0)
        place = jnp.where(iota((128, 256), 0) == rank[:, part], 1.0, 0.0).astype(BF16)
        cells_high += mm_nt((hit * high[:, part]).astype(BF16), place)
        cells_low += mm_nt((hit * low[:, part]).astype(BF16), place)
    cells = (256.0 * cells_high + cells_low).reshape(N_GRP, GRP, 128)
    send_cells[...] = cells
    recv_cells[N_GRP - 1, GRP - 1 :] = cells[N_GRP - 1, GRP - 1 :]

    ins[2].wait()
    where_from = iota((GRP * 32, GLON), 0)
    tile, slot = where_from // 32, where_from % 32
    column = jnp.where(
        slot < TLON,
        tile * TLON + slot,
        jnp.where(
            slot == TLON,
            (tile * TLON + GLON - 1) % GLON,
            jnp.where(slot == TLON + 1, (tile * TLON + TLON) % GLON, -1),
        ),
    )
    pick = jnp.where(column == iota((GRP * 32, GLON), 1), 1.0, 0.0).astype(BF16)
    send_cot[...] = mm(pick, cot_ref[...]).reshape(GRP, 32, CH).astype(BF16)
    recv_cot[1 + lon] = send_cot[lon]

    ins[3].wait()

    def pack(g):
        total = jnp.zeros((SLOTS, FEAT), F32)
        for i in range(OBS // 256):
            part = slice(i * 256, (i + 1) * 256)
            take = jnp.where(iota((SLOTS, 256), 0) + g * SLOTS == key[:, part], 1.0, 0.0)
            total += mm(take.astype(BF16), obs_ref[part, :])
        send_rows[g * GRP : (g + 1) * GRP] = total.reshape(GRP, CAP, FEAT).astype(BF16)

    def send_group(g):
        for j in range(members(g)):
            remote(
                send_rows.at[g * GRP + j], recv_rows.at[g * GRP + j],
                row_send.at[g], row_recv.at[g], *peer(g, j),
            ).start()

    for g in range(EARLY):
        pack(g)

    pl.semaphore_wait(barrier, N_DEV - 1)

    def send_cell(g, j, to_lat, to_lon):
        remote(
            send_cells.at[g, pl.ds(j, 1)], recv_cells.at[g, pl.ds(j, 1)],
            cell_send.at[g], cell_recv.at[g], to_lat, to_lon,
        ).start()

    each_peer(send_cell)
    for j in range(GRP - 1):
        remote(
            send_cot.at[lons[j]], recv_cot.at[1 + lon], cot_send, cot_recv, lat, lons[j]
        ).start()

    @pl.when(up_edge)
    def _():
        for j in range(GRP):
            remote(
                send_cot.at[lons[j]], recv_cot.at[TLAT + 1], edge_send.at[0], edge_recv.at[0],
                lat - 1, lons[j],
            ).start()

    @pl.when(down_edge)
    def _():
        for j in range(GRP):
            remote(
                send_cot.at[lons[j]], recv_cot.at[0], edge_send.at[1], edge_recv.at[1],
                lat + 1, lons[j],
            ).start()

    for g in range(EARLY):
        send_group(g)

    for g in range(EARLY, N_GRP):
        pack(g)
        send_group(g)
    recv_rows[N_DEV - 1] = send_rows[N_DEV - 1]

    for copy in ins[4:]:
        copy.wait()
    w_in_t = w_in_ref[...].astype(F32).T.astype(BF16)
    w_out = w_out_ref[...]
    w_out_t = w_out.astype(F32).T.astype(BF16)
    bias_t = jnp.broadcast_to(bias_ref[...], (128, HID)).T[:, 0:1]
    for g in range(N_GRP):
        wait_got(recv_cells.at[g, pl.ds(0, members(g))], cell_recv.at[g])
    codes = recv_cells[...].reshape(N_DEV, 128)
    high = jnp.where(codes >= 256.0, 1.0, 0.0)
    spread = jnp.where(iota((128, SLOTS), 0) == iota((128, SLOTS), 1) % CAP, 1.0, 0.0).astype(BF16)
    codes = 256.0 * mm(high.astype(BF16), spread) + mm((codes - 256.0 * high).astype(BF16), spread)
    own = iota((GRP, SLOTS), 0) == iota((GRP, SLOTS), 1) // CAP
    for g in range(N_GRP):
        mine = jnp.where(own, codes[g * GRP : (g + 1) * GRP], 0.0)
        cell_of = jnp.sum(mine, axis=0, keepdims=True).astype(I32) - 1
        hit = jnp.where(iota((CELLS, SLOTS), 0) == cell_of, 1.0, 0.0)
        at = g % STEP * SLOTS
        places[g // STEP, :, at : at + SLOTS] = hit.astype(BF16)

    wait_got(recv_cot.at[pl.ds(0, GRP - 1)], cot_recv)

    @pl.when(lat < N_GRP - 1)
    def _():
        wait_got(recv_cot.at[TLAT + 1], edge_recv.at[0])

    @pl.when(lat > 0)
    def _():
        wait_got(recv_cot.at[0], edge_recv.at[1])

    cot_all = recv_cot[...].astype(F32)
    cot_f[:, 8:32, :] = cot_all[:, 0:TLON]
    cot_f[:, 7:8, :] = cot_all[:, TLON : TLON + 1]
    cot_f[:, 32:33, :] = cot_all[:, TLON + 1 : TLON + 2]

    for b in (-1, 0, 1):
        cot_s[b + 1] = cot_f[:, 8 - b : 8 - b + TLON, :]

    def adjoint_row(r, carry):
        total = jnp.zeros((TLON, CH), F32)
        for k, (a, b) in enumerate(TAPS):
            total += taps_ref[k : k + 1, :] * cot_s[b + 1, r + 1 - a]
        send_grid[r] = (SCALE * total).astype(BF16)
        return carry

    lax.fori_loop(0, TLAT, adjoint_row, 0)
    adj_t[...] = send_grid[...].astype(F32).reshape(CELLS, CH).T.astype(BF16)

    for i in range(N_STEP):
        up = mm(adj_t[...], places[i]).astype(BF16)
        ups[i] = up
        backs[i] = mm(w_out, up)

    acc_in[...] = jnp.zeros_like(acc_in)
    acc_out[...] = jnp.zeros_like(acc_out)
    acc_bias[...] = jnp.zeros_like(acc_bias)

    def work(i):
        rows = recv_rows[i * STEP * GRP : (i + 1) * STEP * GRP]
        rows = rows.astype(F32).reshape(WIDE, FEAT).astype(BF16)
        before = mm_nt(w_in_t, rows) + bias_t
        square = before * before
        t = jnp.tanh(C0 * before * (1.0 + C1 * square))
        half = 0.5 * (1.0 + t)
        slope = half + 0.5 * before * (1.0 - t * t) * (C0 * (1.0 + 3.0 * C1 * square))
        hidden = (before * half).astype(BF16)
        pre = (backs[i] * slope).astype(BF16)
        encoded = mm(w_out_t, hidden).astype(BF16)
        add = mm_nt(places[i], encoded).reshape(TLAT, TLON, CH)
        dep[1 : 1 + TLAT, 8 : 8 + TLON, :] += add
        acc_out[...] += mm_nt(hidden, ups[i])
        acc_in[...] += mm(pre, rows)
        pre = pre.astype(F32)
        acc_bias[...] += sum(pre[:, k * 128 : (k + 1) * 128] for k in range(WIDE // 128))

    for i in range(N_STEP):
        for g in range(i * STEP, (i + 1) * STEP):
            wait_got(recv_rows.at[pl.ds(g * GRP, members(g))], row_recv.at[g])
        work(i)

    north, south = lat > 0, lat < N_GRP - 1
    west, east = lax.rem(lon + 15, GRP), lax.rem(lon + 1, GRP)
    core = (1, TLAT)
    first, last = (1, 1), (TLAT, 1)
    above, below = (0, 1), (TLAT + 1, 1)
    wide, left, right = (8, TLON), (8, 1), (8 + TLON - 1, 1)
    before_left, after_right = (7, 1), (8 + TLON, 1)
    halos = [
        (None, lat, west, core, left, core, after_right),
        (None, lat, east, core, right, core, before_left),
        (north, lat - 1, lon, first, wide, below, wide),
        (south, lat + 1, lon, last, wide, above, wide),
        (north, lat - 1, west, first, left, below, after_right),
        (north, lat - 1, east, first, right, below, before_left),
        (south, lat + 1, west, last, left, above, after_right),
        (south, lat + 1, east, last, right, above, before_left),
    ]
    comes = [None, None, south, north, south, south, north, north]

    def at(rows, columns):
        return dep.at[pl.ds(*rows), pl.ds(*columns), :]

    for i, (there, to_lat, to_lon, sr, sc, dr, dc) in enumerate(halos):
        def send_halo(i=i, to_lat=to_lat, to_lon=to_lon, sr=sr, sc=sc, dr=dr, dc=dc):
            remote(
                at(sr, sc), at(dr, dc), halo_send.at[i], halo_recv.at[i], to_lat, to_lon
            ).start()

        send_halo() if there is None else pl.when(there)(send_halo)

    def taps_row(r, totals):
        for at in range(0, TLON, 8):
            mine = dep[r + 1, 8 + at : 16 + at, :]
            totals = tuple(
                total + mine * cot_s[b + 1, r + 1 - a, at : at + 8]
                for total, (a, b) in zip(totals, TAPS)
            )
        return totals

    totals = lax.fori_loop(0, TLAT, taps_row, (jnp.zeros((8, CH), F32),) * 9)
    small = [SCALE * jnp.sum(t, axis=0, keepdims=True) for t in totals]
    small.append(jnp.sum(acc_bias[...].T, axis=0, keepdims=True))
    small = [h for s in small for h in (s[:, :128], s[:, 128:])]
    small = jnp.concatenate(small + [jnp.zeros((4, 128), F32)], axis=0)
    small_high = small.astype(BF16)
    small_low = (small - small_high.astype(F32)).astype(BF16)
    chunks[0:32] = acc_in[...].reshape(32, 8, 128).astype(BF16)
    chunks[32:64] = acc_out[:, :128].reshape(32, 8, 128).astype(BF16)
    chunks[64:96] = acc_out[:, 128:].reshape(32, 8, 128).astype(BF16)
    chunks[96:99] = small_high.astype(F32).reshape(3, 8, 128).astype(BF16)
    chunks[99:102] = small_low.astype(F32).reshape(3, 8, 128).astype(BF16)
    chunks[102:128] = jnp.zeros((26, 8, 128), BF16)

    def send_part(g, j, to_lat, to_lon):
        remote(
            chunks.at[to_lat * GRP + to_lon], parts.at[g * GRP + j],
            part_send.at[g], part_recv.at[g], to_lat, to_lon,
        ).start()

    each_peer(send_part)
    parts[N_DEV - 1] = chunks[me]

    for i, there in enumerate(comes):
        _, _, _, _, _, dr, dc = halos[i]
        def got_halo(i=i, dr=dr, dc=dc):
            wait_got(at(dr, dc), halo_recv.at[i])

        got_halo() if there is None else pl.when(there)(got_halo)

    def grid_row(r, carry):
        total = jnp.zeros((TLON, CH), F32)
        for k, (a, b) in enumerate(TAPS):
            total += taps_ref[k : k + 1, :] * dep[r + 1 + a, 8 + b : 8 + b + TLON, :]
        send_grid[r] = total.astype(BF16)
        return carry

    lax.fori_loop(0, TLAT, grid_row, 0)
    for j in range(GRP - 1):
        remote(
            send_grid.at[lons[j]], grid_ref.at[lon], grid_send, grid_recv, lat, lons[j]
        ).start()
    mine_grid = pltpu.make_async_copy(send_grid.at[lon], grid_ref.at[lon], own_sem.at[0])
    mine_grid.start()

    for g in range(N_GRP):
        wait_got(parts.at[pl.ds(g * GRP, members(g))], part_recv.at[g])
    mine = jnp.sum(parts[...].astype(F32), axis=0).astype(BF16)
    red[...] = mine
    mine_share = pltpu.make_async_copy(red, shared.at[me], own_sem.at[1])
    mine_share.start()

    def send_share(g, j, to_lat, to_lon):
        remote(
            red, shared.at[me], share_send.at[g], share_recv.at[g], to_lat, to_lon
        ).start()

    each_peer(send_share)

    for g in range(N_GRP):
        wait_got(shared.at[pl.ds(g * GRP, members(g))], share_recv.at[g])
    mine_grid.wait()
    mine_share.wait()
    wait_got(grid_ref.at[pl.ds(0, GRP - 1)], grid_recv)
    for g in range(N_GRP):
        n = members(g)
        wait_sent(send_cells.at[g, pl.ds(0, n)], cell_send.at[g])
        wait_sent(send_rows.at[pl.ds(g * GRP, n)], row_send.at[g])
        wait_sent(chunks.at[pl.ds(g * GRP, n)], part_send.at[g])
        wait_sent(shared.at[pl.ds(g * GRP, n)], share_send.at[g])
    wait_sent(send_cot.at[pl.ds(0, GRP - 1)], cot_send)
    wait_sent(send_grid.at[pl.ds(0, GRP - 1)], grid_send)

    @pl.when(up_edge)
    def _():
        wait_sent(send_cot, edge_send.at[0])

    @pl.when(down_edge)
    def _():
        wait_sent(send_cot, edge_send.at[1])

    for i, (there, _, _, sr, sc, _, _) in enumerate(halos):
        def sent_halo(i=i, sr=sr, sc=sc):
            wait_sent(at(sr, sc), halo_send.at[i])

        sent_halo() if there is None else pl.when(there)(sent_halo)


def finish(
    grid_in, shared_in, grid_hbm, g_in_hbm, g_bias_hbm, g_out_hbm, g_taps_hbm,
    grid, shared, g_in, g_bias, g_out, g_taps, sem,
):
    come = pltpu.make_async_copy(shared_in, shared, sem.at[5])
    come.start()
    grid_come = pltpu.make_async_copy(grid_in, grid, sem.at[6])
    grid_come.start()
    copies = [pltpu.make_async_copy(grid, grid_hbm, sem.at[0])]
    come.wait()
    g_out[:, :128] = shared[32:64].astype(F32).reshape(HID, 128)
    g_out[:, 128:] = shared[64:96].astype(F32).reshape(HID, 128)
    copies.append(pltpu.make_async_copy(g_out, g_out_hbm, sem.at[1]))
    copies[1].start()
    g_in[...] = shared[0:32].astype(F32).reshape(HID, FEAT).T
    copies.append(pltpu.make_async_copy(g_in, g_in_hbm, sem.at[2]))
    copies[2].start()
    grid_come.wait()
    copies[0].start()
    small = (shared[96:99].astype(F32) + shared[99:102].astype(F32)).reshape(24, 128)
    for k in range(9):
        g_taps[k : k + 1, :128] = small[2 * k : 2 * k + 1]
        g_taps[k : k + 1, 128:] = small[2 * k + 1 : 2 * k + 2]
    g_bias[:, :128] = small[18:19]
    g_bias[:, 128:] = small[19:20]
    copies.append(pltpu.make_async_copy(g_taps, g_taps_hbm, sem.at[3]))
    copies.append(pltpu.make_async_copy(g_bias, g_bias_hbm, sem.at[4]))
    copies[3].start()
    copies[4].start()
    for copy in copies:
        copy.wait()


def local(obs, owner, cell, count, w_in, bias, w_out, taps, cot):
    smem = pl.BlockSpec(memory_space=pltpu.SMEM)
    hbm = pl.BlockSpec(memory_space=pltpu.HBM)
    dma = pltpu.SemaphoreType.DMA
    rows, shared = pl.pallas_call(
        kernel,
        name="encode_step",
        out_shape=(
            jax.ShapeDtypeStruct((GRP, TLON, CH), BF16),
            jax.ShapeDtypeStruct((N_DEV, 8, 128), BF16),
        ),
        in_specs=[hbm, hbm, hbm, smem, hbm, hbm, hbm, hbm, hbm],
        out_specs=(hbm,) * 2,
        scratch_shapes=[
            pltpu.VMEM((OBS, FEAT), BF16),
            pltpu.VMEM((1, OBS), I32),
            pltpu.VMEM((OBS,), I32),
            pltpu.VMEM((FEAT, HID), BF16),
            pltpu.VMEM((1, HID), F32),
            pltpu.VMEM((HID, CH), BF16),
            pltpu.VMEM((9, CH), F32),
            pltpu.VMEM((GLON, CH), BF16),
            pltpu.VMEM((N_DEV, CAP, FEAT), BF16),
            pltpu.VMEM((N_DEV, CAP, FEAT), BF16),
            pltpu.VMEM((N_GRP, GRP, 128), F32),
            pltpu.VMEM((N_GRP, GRP, 128), F32),
            pltpu.VMEM((GRP, 32, CH), BF16),
            pltpu.VMEM((TLAT + 2, 32, CH), BF16),
            pltpu.VMEM((TLAT + 2, 40, CH), F32),
            pltpu.VMEM((3, TLAT + 2, TLON, CH), F32),
            pltpu.VMEM((TLAT + 2, 40, CH), F32),
            pltpu.VMEM((TLAT, TLON, CH), BF16),
            pltpu.VMEM((N_DEV, 8, 128), BF16),
            pltpu.VMEM((N_DEV, 8, 128), BF16),
            pltpu.VMEM((8, 128), BF16),
            pltpu.VMEM((HID, FEAT), F32),
            pltpu.VMEM((HID, CH), F32),
            pltpu.VMEM((HID, 128), F32),
            pltpu.VMEM((CH, CELLS), BF16),
            pltpu.VMEM((N_STEP, CELLS, WIDE), BF16),
            pltpu.VMEM((N_STEP, HID, WIDE), BF16),
            pltpu.VMEM((N_STEP, HID, WIDE), F32),
            dma((8,)), dma((2,)),
            dma((N_GRP,)), dma((N_GRP,)), dma((N_GRP,)), dma((N_GRP,)),
            dma, dma, dma((2,)), dma((2,)),
            dma((N_GRP,)), dma((N_GRP,)), dma((N_GRP,)), dma((N_GRP,)),
            dma((8,)), dma((8,)), dma, dma,
        ],
        compiler_params=pltpu.CompilerParams(
            collective_id=0, has_side_effects=True, vmem_limit_bytes=67043328
        ),
        cost_estimate=pl.CostEstimate(
            flops=4_000_000_000, bytes_accessed=2_000_000, transcendentals=800_000
        ),
    )(
        obs, owner.reshape(1, OBS), cell, count, w_in, bias.reshape(1, HID),
        w_out, taps, cot.reshape(GLON, CH),
    )
    outs = [((GRP, TLON, CH), BF16), ((FEAT, HID), F32), ((1, HID), F32), ((HID, CH), F32), ((9, CH), F32)]
    grid, g_in, g_bias, g_out, g_taps = pl.pallas_call(
        finish,
        name="finish",
        out_shape=tuple(jax.ShapeDtypeStruct(*o) for o in outs),
        in_specs=[hbm, hbm],
        out_specs=(hbm,) * 5,
        scratch_shapes=[
            pltpu.VMEM(*outs[0]),
            pltpu.VMEM((N_DEV, 8, 128), BF16),
            *[pltpu.VMEM(*o) for o in outs[1:]],
            dma((7,)),
        ],
        compiler_params=pltpu.CompilerParams(vmem_limit_bytes=67043328),
    )(rows, shared)
    return (grid.reshape(1, GLON, CH), g_in, g_bias.reshape(HID), g_out, g_taps)


def solution(mesh):
    block = P(("lat", "lon"))
    return jax.shard_map(
        local,
        mesh=mesh,
        in_specs=(block, block, block, block, P(), P(), P(), P(), block),
        out_specs=(block, P(), P(), P(), P()),
        check_vma=False,
    )
```

```python
import functools
import math

import jax
import jax.numpy as jnp
import numpy as np
from jax import lax
from jax.experimental import pallas as pl
from jax.experimental.pallas import tpu as pltpu
from jax.sharding import PartitionSpec as P

MESH = pl.DeviceIdType.MESH
F32, BF16, I32 = jnp.float32, jnp.bfloat16, jnp.int32
NT = (((1,), (1,)), ((), ()))
TAPS = [(a, b) for a in (-1, 0, 1) for b in (-1, 0, 1)]

N_DEV, N_GRP, GRP = 128, 8, 16
EARLY = 3
HOLD = 7
STEPS = ((0, 1), (2, 3), (4, 5), (6, 7))
OBS, FEAT, HID, CH = 1536, 128, 256, 256
CAP = 24
SLOTS = GRP * CAP
TLAT, TLON = 16, 24
CELLS = TLAT * TLON
GLON = 384
CHUNKS_IN, CHUNKS_OUT, CHUNKS_SMALL = 32, 64, 3
SCALE = 1.0 / math.sqrt(OBS * N_DEV)
C0, C1 = math.sqrt(2.0 / math.pi), 0.044715


def iota(shape, dim):
    return lax.broadcasted_iota(I32, shape, dim)


def mm(a, b):
    return jnp.dot(a, b, preferred_element_type=F32)


def mm_nt(a, b):
    return lax.dot_general(a, b, NT, preferred_element_type=F32)


def hops(offset):
    dz, dc, dx, dy = offset
    return sum(min(d, 4 - d) for d in (dz, dx, dy)) + 0.1 * dc


PLACES = sorted(
    ((i // 32, i // 16 % 2, i // 4 % 4, i % 4) for i in range(N_DEV)), key=hops, reverse=True
)


def kernel(
    obs_hbm, owner_hbm, cell_hbm, count_hbm, order_hbm, w_in_hbm, bias_hbm, w_out_hbm, taps_hbm, cot_hbm,
    grid_ref, shared,
    obs_ref, owner_ref, cell_ref, count_ref, order_ref, w_in_ref, bias_ref, w_out_ref, taps_ref, cot_ref,
    send_rows, recv_rows, send_cells, recv_cells, send_cot, recv_cot, cot_f, cot_s, dep, send_grid,
    chunks, parts, red, acc_in, acc_out, adj_t, places, ups, backs,
    in_sem, own_sem,
    row_send, row_recv, cell_send, cell_recv, cot_send, cot_recv, edge_send, edge_recv,
    part_send, part_recv, share_send, share_recv, halo_send, halo_recv, grid_send, grid_recv,
):
    ins = [
        pltpu.make_async_copy(src, dst, in_sem.at[i])
        for i, (src, dst) in enumerate([
            (owner_hbm, owner_ref), (count_hbm, count_ref), (order_hbm, order_ref), (cell_hbm, cell_ref), (cot_hbm, cot_ref), (obs_hbm, obs_ref),
            (w_in_hbm, w_in_ref), (w_out_hbm, w_out_ref), (bias_hbm, bias_ref), (taps_hbm, taps_ref),
        ])
    ]
    for copy in ins:
        copy.start()

    lat, lon = lax.axis_index("lat"), lax.axis_index("lon")
    z, c, x, y = lax.div(lat, 2), lax.rem(lat, 2), lax.div(lon, 4), lax.rem(lon, 4)
    me = lat * GRP + lon
    up_edge = (lat > 0) & (lon == 0)
    down_edge = (lat < N_GRP - 1) & (lon == GRP - 1)
    zs, cs, xs, ys = ([lax.rem(at + d, n) for d in range(n)] for at, n in ((z, 4), (c, 2), (x, 4), (y, 4)))

    def peer(g, j):
        dz, dc, dx, dy = PLACES[g * GRP + j]
        return zs[dz] * 2 + cs[dc], xs[dx] * 4 + ys[dy]

    plane = [d for d in PLACES if d[:2] == (0, 0)]
    lons = [xs[dx] * 4 + ys[dy] for _, _, dx, dy in plane]

    def members(g):
        return GRP if g < N_GRP - 1 else GRP - 1

    def each_peer(fn):
        for g in range(N_GRP):
            for j in range(members(g)):
                fn(g, j, *peer(g, j))

    def remote(src, dst, send, recv, to_lat, to_lon):
        return pltpu.make_async_remote_copy(
            src_ref=src, dst_ref=dst, send_sem=send, recv_sem=recv,
            device_id=(to_lat, to_lon), device_id_type=MESH,
        )

    def wait_sent(ref, sem):
        remote(ref, ref, sem, sem, lat, lon).wait_send()

    def wait_got(ref, sem):
        remote(ref, ref, sem, sem, lat, lon).wait_recv()


    dep[...] = jnp.zeros_like(dep)
    recv_cot[0] = jnp.zeros(recv_cot.shape[1:], BF16)
    recv_cot[TLAT + 1] = jnp.zeros(recv_cot.shape[1:], BF16)

    barrier = pltpu.get_barrier_semaphore()

    def greet(g, j, to_lat, to_lon):
        pl.semaphore_signal(barrier, inc=1, device_id=(to_lat, to_lon), device_id_type=MESH)

    each_peer(greet)


    for copy in ins[:4]:
        copy.wait()
    owner = owner_ref[...]
    valid = iota((1, OBS), 1) < count_ref[0]
    o_lat, o_lon = owner // GRP, owner % GRP
    dz, dc = (o_lat // 2 - z + 4) % 4, (o_lat - c + 2) % 2
    dx, dy = (o_lon // 4 - x + 4) % 4, (o_lon - y + 4) % 4
    rel = dz * 32 + dc * 16 + dx * 4 + dy
    rel = jnp.where(valid, rel, -1)
    upto = jnp.where(iota((256, 256), 0) <= iota((256, 256), 1), 1.0, 0.0).astype(BF16)
    order = jnp.concatenate([order_ref[...]] * 2, axis=1)
    base = (iota((N_DEV, 256), 0) * CAP).astype(F32)
    carry = jnp.zeros((N_DEV, 1), F32)
    ranks, keys, hits = [], [], []
    for i in range(OBS // 256):
        hit = jnp.where(order == rel[:, i * 256 : (i + 1) * 256], 1.0, 0.0)
        count = mm(hit.astype(BF16), upto) + carry
        ranks.append(jnp.sum(hit * count, axis=0, keepdims=True) - 1.0)
        keys.append(jnp.sum(hit * (count + base), axis=0, keepdims=True) - 1.0)
        carry = count[:, 255:256]
        hits.append(hit)
    rank = jnp.concatenate(ranks, axis=1).astype(I32)
    key = jnp.concatenate(keys, axis=1).astype(I32)


    value = cell_ref[...].reshape(1, OBS) + 1
    high = jnp.where(value >= 256, 1.0, 0.0)
    low = value.astype(F32) - 256.0 * high
    cells_high = jnp.zeros((N_DEV, 128), F32)
    cells_low = jnp.zeros((N_DEV, 128), F32)
    for i in range(OBS // 256):
        part = slice(i * 256, (i + 1) * 256)
        hit = hits[i]
        place = jnp.where(iota((128, 256), 0) == rank[:, part], 1.0, 0.0).astype(BF16)
        cells_high += mm_nt((hit * high[:, part]).astype(BF16), place)
        cells_low += mm_nt((hit * low[:, part]).astype(BF16), place)
    cells = (256.0 * cells_high + cells_low).reshape(N_GRP, GRP, 128)
    send_cells[...] = cells
    recv_cells[N_GRP - 1, GRP - 1 :] = cells[N_GRP - 1, GRP - 1 :]


    ins[4].wait()
    where_from = iota((GRP * 32, GLON), 0)
    tile, slot = where_from // 32, where_from % 32
    column = jnp.where(
        slot < TLON,
        tile * TLON + slot,
        jnp.where(
            slot == TLON,
            (tile * TLON + GLON - 1) % GLON,
            jnp.where(slot == TLON + 1, (tile * TLON + TLON) % GLON, -1),
        ),
    )
    pick = jnp.where(column == iota((GRP * 32, GLON), 1), 1.0, 0.0).astype(BF16)
    send_cot[...] = mm(pick, cot_ref[...]).reshape(GRP, 32, CH)[:, :26].astype(BF16)
    recv_cot[1 + lon] = send_cot[lon]


    ins[5].wait()

    def pack(g):
        total = jnp.zeros((SLOTS, FEAT), F32)
        for i in range(OBS // 256):
            part = slice(i * 256, (i + 1) * 256)
            take = jnp.where(iota((SLOTS, 256), 0) + g * SLOTS == key[:, part], 1.0, 0.0)
            total += mm(take.astype(BF16), obs_ref[part, :])
        send_rows[g * GRP : (g + 1) * GRP] = total.reshape(GRP, CAP, FEAT).astype(BF16)

    def send_group(g):
        for j in range(members(g)):
            remote(
                send_rows.at[g * GRP + j], recv_rows.at[g * GRP + j],
                row_send.at[g], row_recv.at[g], *peer(g, j),
            ).start()

    for g in range(EARLY):
        pack(g)


    pl.semaphore_wait(barrier, N_DEV - 1)


    def send_cell(g, j, to_lat, to_lon):
        remote(
            send_cells.at[g, pl.ds(j, 1)], recv_cells.at[g, pl.ds(j, 1)],
            cell_send.at[g], cell_recv.at[g], to_lat, to_lon,
        ).start()

    each_peer(send_cell)
    for j in range(GRP - 1):
        remote(
            send_cot.at[lons[j]], recv_cot.at[1 + lon], cot_send, cot_recv, lat, lons[j]
        ).start()

    @pl.when(up_edge)
    def _():
        for j in range(GRP):
            remote(
                send_cot.at[lons[j]], recv_cot.at[TLAT + 1], edge_send.at[0], edge_recv.at[0],
                lat - 1, lons[j],
            ).start()

    @pl.when(down_edge)
    def _():
        for j in range(GRP):
            remote(
                send_cot.at[lons[j]], recv_cot.at[0], edge_send.at[1], edge_recv.at[1],
                lat + 1, lons[j],
            ).start()


    for g in range(EARLY, HOLD):
        pack(g)
    for g in range(HOLD):
        send_group(g)
    for g in range(HOLD, N_GRP):
        pack(g)
        send_group(g)
    recv_rows[N_DEV - 1] = send_rows[N_DEV - 1]


    for copy in ins[6:]:
        copy.wait()
    w_in_t = w_in_ref[...].astype(F32).T.astype(BF16)
    w_out = w_out_ref[...]
    w_out_t = w_out.astype(F32).T.astype(BF16)
    bias_t = jnp.broadcast_to(bias_ref[...], (128, HID)).T[:, 0:1]
    for g in range(N_GRP):
        wait_got(recv_cells.at[g, pl.ds(0, members(g))], cell_recv.at[g])
    codes = recv_cells[...].reshape(N_DEV, 128)
    high = jnp.where(codes >= 256.0, 1.0, 0.0)
    spread = jnp.where(iota((128, SLOTS), 0) == iota((128, SLOTS), 1) % CAP, 1.0, 0.0).astype(BF16)
    codes = 256.0 * mm(high.astype(BF16), spread) + mm((codes - 256.0 * high).astype(BF16), spread)
    own = iota((GRP, SLOTS), 0) == iota((GRP, SLOTS), 1) // CAP

    for g in range(N_GRP):
        mine = jnp.where(own, codes[g * GRP : (g + 1) * GRP], 0.0)
        cell_of = jnp.sum(mine, axis=0, keepdims=True).astype(I32) - 1
        hit = jnp.where(iota((CELLS, SLOTS), 0) == cell_of, 1.0, 0.0)
        places[:, g * SLOTS : (g + 1) * SLOTS] = hit.astype(BF16)


    wait_got(recv_cot.at[pl.ds(0, GRP - 1)], cot_recv)


    def spread_cot(rows):
        part = recv_cot[rows].astype(F32)
        cot_f[rows, 8:32, :] = part[:, 0:TLON]
        cot_f[rows, 7:8, :] = part[:, TLON : TLON + 1]
        cot_f[rows, 32:33, :] = part[:, TLON + 1 : TLON + 2]
        for b in (-1, 0, 1):
            cot_s[b + 1, rows] = cot_f[rows, 8 - b : 8 - b + TLON, :]

    def adjoint_row(r, carry):
        total = jnp.zeros((TLON, CH), F32)
        for k, (a, b) in enumerate(TAPS):
            total += taps_ref[k : k + 1, :] * cot_s[b + 1, r + 1 - a]
        send_grid[r] = (SCALE * total).astype(BF16)
        return carry

    spread_cot(slice(1, TLAT + 1))
    lax.fori_loop(1, TLAT - 1, adjoint_row, 0)


    @pl.when(lat < N_GRP - 1)
    def _():
        wait_got(recv_cot.at[TLAT + 1], edge_recv.at[0])

    @pl.when(lat > 0)
    def _():
        wait_got(recv_cot.at[0], edge_recv.at[1])


    for row in (0, TLAT + 1):
        spread_cot(slice(row, row + 1))
    adjoint_row(0, 0)
    adjoint_row(TLAT - 1, 0)
    adj_t[...] = send_grid[...].astype(F32).reshape(CELLS, CH).T.astype(BF16)


    for i in range(0, N_GRP, 2):
        at = slice(i * SLOTS, (i + 2) * SLOTS)
        up = mm(adj_t[...], places[:, at]).astype(BF16)
        ups[:, at] = up
        backs[:, at] = mm(w_out, up)

    acc_in[...] = jnp.zeros_like(acc_in)
    acc_out[...] = jnp.zeros_like(acc_out)

    def work(groups):
        start, count = groups[0], len(groups)
        at = slice(start * SLOTS, (start + count) * SLOTS)
        rows = recv_rows[start * GRP : (start + count) * GRP]
        rows = rows.astype(F32).reshape(count * SLOTS, FEAT).astype(BF16)
        before = mm_nt(w_in_t, rows) + bias_t
        square = before * before
        half = 0.5 + 0.5 * jnp.tanh(before * (C0 + C0 * C1 * square))
        value = before * half
        hidden = value.astype(BF16)
        slope = half + value * (1.0 - half) * (2.0 * C0 + 6.0 * C0 * C1 * square)
        pre = (backs[:, at] * slope).astype(BF16)
        encoded = mm(w_out_t, hidden).astype(BF16)
        add = mm_nt(places[:, at], encoded).reshape(TLAT, TLON, CH)
        dep[1 : 1 + TLAT, 8 : 8 + TLON, :] += add
        acc_out[...] += mm_nt(hidden, ups[:, at])
        ones = jnp.ones((count * SLOTS, 128), BF16)
        acc_in[...] += mm(pre, jnp.concatenate([rows, ones], axis=1))

    for groups in STEPS:
        for g in groups:
            wait_got(recv_rows.at[pl.ds(g * GRP, members(g))], row_recv.at[g])
        work(groups)


    north, south = lat > 0, lat < N_GRP - 1
    west, east = lax.rem(lon + 15, GRP), lax.rem(lon + 1, GRP)
    core = (1, TLAT)
    first, last = (1, 1), (TLAT, 1)
    above, below = (0, 1), (TLAT + 1, 1)
    wide, left, right = (8, TLON), (8, 1), (8 + TLON - 1, 1)
    before_left, after_right = (7, 1), (8 + TLON, 1)
    halos = [
        (None, lat, west, core, left, core, after_right),
        (None, lat, east, core, right, core, before_left),
        (north, lat - 1, lon, first, wide, below, wide),
        (south, lat + 1, lon, last, wide, above, wide),
        (north, lat - 1, west, first, left, below, after_right),
        (north, lat - 1, east, first, right, below, before_left),
        (south, lat + 1, west, last, left, above, after_right),
        (south, lat + 1, east, last, right, above, before_left),
    ]
    comes = [None, None, south, north, south, south, north, north]

    def at(rows, columns):
        return dep.at[pl.ds(*rows), pl.ds(*columns), :]

    for i, (there, to_lat, to_lon, sr, sc, dr, dc) in enumerate(halos):
        def send_halo(i=i, to_lat=to_lat, to_lon=to_lon, sr=sr, sc=sc, dr=dr, dc=dc):
            remote(
                at(sr, sc), at(dr, dc), halo_send.at[i], halo_recv.at[i], to_lat, to_lon
            ).start()

        send_halo() if there is None else pl.when(there)(send_halo)


    def taps_row(r, totals):
        for at in range(0, TLON, 8):
            mine = dep[r + 1, 8 + at : 16 + at, :]
            totals = tuple(
                total + mine * cot_s[b + 1, r + 1 - a, at : at + 8]
                for total, (a, b) in zip(totals, TAPS)
            )
        return totals

    totals = lax.fori_loop(0, TLAT, taps_row, (jnp.zeros((8, CH), F32),) * 9)
    small = [SCALE * jnp.sum(t, axis=0, keepdims=True) for t in totals]
    small.append(acc_in[:, FEAT:].T[0:1])
    small = [h for s in small for h in (s[:, :128], s[:, 128:])]
    small = jnp.concatenate(small + [jnp.zeros((4, 128), F32)], axis=0)
    small_high = small.astype(BF16)
    small_low = (small - small_high.astype(F32)).astype(BF16)

    chunks[0:32] = acc_in[:, :FEAT].reshape(32, 8, 128).astype(BF16)
    chunks[32:64] = acc_out[:, :128].reshape(32, 8, 128).astype(BF16)
    chunks[64:96] = acc_out[:, 128:].reshape(32, 8, 128).astype(BF16)
    chunks[96:99] = small_high.astype(F32).reshape(3, 8, 128).astype(BF16)
    chunks[99:102] = small_low.astype(F32).reshape(3, 8, 128).astype(BF16)
    chunks[102:128] = jnp.zeros((26, 8, 128), BF16)

    def send_part(g, j, to_lat, to_lon):
        remote(
            chunks.at[to_lat * GRP + to_lon], parts.at[g * GRP + j],
            part_send.at[g], part_recv.at[g], to_lat, to_lon,
        ).start()


    each_peer(send_part)
    parts[N_DEV - 1] = chunks[me]


    for i, there in enumerate(comes):
        _, _, _, _, _, dr, dc = halos[i]
        def got_halo(i=i, dr=dr, dc=dc):
            wait_got(at(dr, dc), halo_recv.at[i])

        got_halo() if there is None else pl.when(there)(got_halo)


    def grid_row(r, carry):
        total = jnp.zeros((TLON, CH), F32)
        for k, (a, b) in enumerate(TAPS):
            total += taps_ref[k : k + 1, :] * dep[r + 1 + a, 8 + b : 8 + b + TLON, :]
        send_grid[r] = total.astype(BF16)
        return carry

    lax.fori_loop(0, TLAT, grid_row, 0)
    for j in range(GRP - 1):
        remote(
            send_grid.at[lons[j]], grid_ref.at[lon], grid_send, grid_recv, lat, lons[j]
        ).start()
    mine_grid = pltpu.make_async_copy(send_grid.at[lon], grid_ref.at[lon], own_sem.at[0])
    mine_grid.start()


    for g in range(N_GRP):
        wait_got(parts.at[pl.ds(g * GRP, members(g))], part_recv.at[g])

    mine = jnp.sum(parts[...].astype(F32), axis=0).astype(BF16)
    red[...] = mine
    mine_share = pltpu.make_async_copy(red, shared.at[me], own_sem.at[1])
    mine_share.start()

    def send_share(g, j, to_lat, to_lon):
        remote(
            red, shared.at[me], share_send.at[g], share_recv.at[g], to_lat, to_lon
        ).start()


    each_peer(send_share)


    for g in range(N_GRP):
        wait_got(shared.at[pl.ds(g * GRP, members(g))], share_recv.at[g])

    mine_grid.wait()
    mine_share.wait()
    wait_got(grid_ref.at[pl.ds(0, GRP - 1)], grid_recv)
    for g in range(N_GRP):
        n = members(g)
        wait_sent(send_cells.at[g, pl.ds(0, n)], cell_send.at[g])
        wait_sent(send_rows.at[pl.ds(g * GRP, n)], row_send.at[g])
        wait_sent(chunks.at[pl.ds(g * GRP, n)], part_send.at[g])
        wait_sent(shared.at[pl.ds(g * GRP, n)], share_send.at[g])
    wait_sent(send_cot.at[pl.ds(0, GRP - 1)], cot_send)
    wait_sent(send_grid.at[pl.ds(0, GRP - 1)], grid_send)

    @pl.when(up_edge)
    def _():
        wait_sent(send_cot, edge_send.at[0])

    @pl.when(down_edge)
    def _():
        wait_sent(send_cot, edge_send.at[1])

    for i, (there, _, _, sr, sc, _, _) in enumerate(halos):
        def sent_halo(i=i, sr=sr, sc=sc):
            wait_sent(at(sr, sc), halo_send.at[i])

        sent_halo() if there is None else pl.when(there)(sent_halo)


def finish(
    grid_in, shared_in, grid_hbm, g_in_hbm, g_bias_hbm, g_out_hbm, g_taps_hbm,
    grid, shared, g_in, g_bias, g_out, g_taps, sem,
):
    come = pltpu.make_async_copy(shared_in, shared, sem.at[5])
    come.start()
    grid_come = pltpu.make_async_copy(grid_in, grid, sem.at[6])
    grid_come.start()
    copies = [pltpu.make_async_copy(grid, grid_hbm, sem.at[0])]
    come.wait()
    g_out[:, :128] = shared[32:64].astype(F32).reshape(HID, 128)
    g_out[:, 128:] = shared[64:96].astype(F32).reshape(HID, 128)
    copies.append(pltpu.make_async_copy(g_out, g_out_hbm, sem.at[1]))
    copies[1].start()
    g_in[...] = shared[0:32].astype(F32).reshape(HID, FEAT).T
    copies.append(pltpu.make_async_copy(g_in, g_in_hbm, sem.at[2]))
    copies[2].start()
    grid_come.wait()
    copies[0].start()
    small = (shared[96:99].astype(F32) + shared[99:102].astype(F32)).reshape(24, 128)
    for k in range(9):
        g_taps[k : k + 1, :128] = small[2 * k : 2 * k + 1]
        g_taps[k : k + 1, 128:] = small[2 * k + 1 : 2 * k + 2]
    g_bias[:, :128] = small[18:19]
    g_bias[:, 128:] = small[19:20]
    copies.append(pltpu.make_async_copy(g_taps, g_taps_hbm, sem.at[3]))
    copies.append(pltpu.make_async_copy(g_bias, g_bias_hbm, sem.at[4]))
    copies[3].start()
    copies[4].start()
    for copy in copies:
        copy.wait()


def local(obs, owner, cell, count, w_in, bias, w_out, taps, cot):
    hbm = pl.BlockSpec(memory_space=pltpu.HBM)
    dma = pltpu.SemaphoreType.DMA
    order = [dz * 32 + dc * 16 + dx * 4 + dy for dz, dc, dx, dy in PLACES]
    order = jnp.asarray(np.repeat(np.array(order, np.int32)[:, None], 128, axis=1))
    rows, shared = pl.pallas_call(
        kernel,
        name="encode_step",
        out_shape=(
            jax.ShapeDtypeStruct((GRP, TLON, CH), BF16),
            jax.ShapeDtypeStruct((N_DEV, 8, 128), BF16),
        ),
        in_specs=[hbm] * 10,
        out_specs=(hbm,) * 2,
        scratch_shapes=[
            pltpu.VMEM((OBS, FEAT), BF16),
            pltpu.VMEM((1, OBS), I32),
            pltpu.VMEM((OBS,), I32),
            pltpu.SMEM((1,), I32),
            pltpu.VMEM((N_DEV, 128), I32),
            pltpu.VMEM((FEAT, HID), BF16),
            pltpu.VMEM((1, HID), F32),
            pltpu.VMEM((HID, CH), BF16),
            pltpu.VMEM((9, CH), F32),
            pltpu.VMEM((GLON, CH), BF16),
            pltpu.VMEM((N_DEV, CAP, FEAT), BF16),
            pltpu.VMEM((N_DEV, CAP, FEAT), BF16),
            pltpu.VMEM((N_GRP, GRP, 128), F32),
            pltpu.VMEM((N_GRP, GRP, 128), F32),
            pltpu.VMEM((GRP, 26, CH), BF16),
            pltpu.VMEM((TLAT + 2, 26, CH), BF16),
            pltpu.VMEM((TLAT + 2, 40, CH), F32),
            pltpu.VMEM((3, TLAT + 2, TLON, CH), F32),
            pltpu.VMEM((TLAT + 2, 40, CH), F32),
            pltpu.VMEM((TLAT, TLON, CH), BF16),
            pltpu.VMEM((N_DEV, 8, 128), BF16),
            pltpu.VMEM((N_DEV, 8, 128), BF16),
            pltpu.VMEM((8, 128), BF16),
            pltpu.VMEM((HID, 2 * FEAT), F32),
            pltpu.VMEM((HID, CH), F32),
            pltpu.VMEM((CH, CELLS), BF16),
            pltpu.VMEM((CELLS, N_GRP * SLOTS), BF16),
            pltpu.VMEM((CH, N_GRP * SLOTS), BF16),
            pltpu.VMEM((HID, N_GRP * SLOTS), F32),
            dma((10,)), dma((2,)),
            dma((N_GRP,)), dma((N_GRP,)), dma((N_GRP,)), dma((N_GRP,)),
            dma, dma, dma((2,)), dma((2,)),
            dma((N_GRP,)), dma((N_GRP,)), dma((N_GRP,)), dma((N_GRP,)),
            dma((8,)), dma((8,)), dma, dma,
        ],
        compiler_params=pltpu.CompilerParams(
            collective_id=0, has_side_effects=True, vmem_limit_bytes=67043328
        ),
        cost_estimate=pl.CostEstimate(
            flops=4_000_000_000, bytes_accessed=2_000_000, transcendentals=800_000
        ),
    )(
        obs, owner.reshape(1, OBS), cell, count, order, w_in, bias.reshape(1, HID),
        w_out, taps, cot.reshape(GLON, CH),
    )
    outs = [((GRP, TLON, CH), BF16), ((FEAT, HID), F32), ((1, HID), F32), ((HID, CH), F32), ((9, CH), F32)]
    grid, g_in, g_bias, g_out, g_taps = pl.pallas_call(
        finish,
        name="finish",
        out_shape=tuple(jax.ShapeDtypeStruct(*o) for o in outs),
        in_specs=[hbm, hbm],
        out_specs=(hbm,) * 5,
        scratch_shapes=[
            pltpu.VMEM(*outs[0]),
            pltpu.VMEM((N_DEV, 8, 128), BF16),
            *[pltpu.VMEM(*o) for o in outs[1:]],
            dma((7,)),
        ],
        compiler_params=pltpu.CompilerParams(vmem_limit_bytes=67043328),
    )(rows, shared)
    return (grid.reshape(1, GLON, CH), g_in, g_bias.reshape(HID), g_out, g_taps)


def solution(mesh):
    block = P(("lat", "lon"))
    return jax.shard_map(
        local,
        mesh=mesh,
        in_specs=(block, block, block, block, P(), P(), P(), P(), block),
        out_specs=(block, P(), P(), P(), P()),
        check_vma=False,
    )
```

```python
import functools
import math

import jax
import jax.numpy as jnp
import numpy as np
from jax import lax
from jax.experimental import pallas as pl
from jax.experimental.pallas import tpu as pltpu
from jax.sharding import PartitionSpec as P

MESH = pl.DeviceIdType.MESH
F32, BF16, I32 = jnp.float32, jnp.bfloat16, jnp.int32
NT = (((1,), (1,)), ((), ()))
TAPS = [(a, b) for a in (-1, 0, 1) for b in (-1, 0, 1)]

N_DEV, N_GRP, GRP = 128, 8, 16
EARLY = 3
HOLD = 7
STEPS = ((0, 1), (2, 3), (4, 5, 6, 7))
OBS, FEAT, HID, CH = 1536, 128, 256, 256
CAP = 24
SLOTS = GRP * CAP
TLAT, TLON = 16, 24
CELLS = TLAT * TLON
GLON = 384
CHUNKS_IN, CHUNKS_OUT, CHUNKS_SMALL = 32, 64, 3
SCALE = 1.0 / math.sqrt(OBS * N_DEV)
C0, C1 = math.sqrt(2.0 / math.pi), 0.044715


def iota(shape, dim):
    return lax.broadcasted_iota(I32, shape, dim)


def mm(a, b):
    return jnp.dot(a, b, preferred_element_type=F32)


def mm_nt(a, b):
    return lax.dot_general(a, b, NT, preferred_element_type=F32)


def hops(offset):
    dz, dc, dx, dy = offset
    return sum(min(d, 4 - d) for d in (dz, dx, dy)) + 0.1 * dc


PLACES = sorted(
    ((i // 32, i // 16 % 2, i // 4 % 4, i % 4) for i in range(N_DEV)), key=hops, reverse=True
)


def kernel(
    obs_hbm, owner_hbm, cell_hbm, count_hbm, order_hbm, w_in_hbm, bias_hbm, w_out_hbm, taps_hbm, cot_hbm,
    grid_ref, shared,
    obs_ref, owner_ref, cell_ref, count_ref, order_ref, w_in_ref, bias_ref, w_out_ref, taps_ref, cot_ref,
    send_rows, recv_rows, send_cells, recv_cells, send_cot, recv_cot, cot_f, cot_s, dep, send_grid,
    chunks, parts, red, acc_in, acc_out, adj_t, places, ups, backs,
    in_sem, own_sem,
    row_send, row_recv, cell_send, cell_recv, cot_send, cot_recv, edge_send, edge_recv,
    part_send, part_recv, share_send, share_recv, halo_send, halo_recv, grid_send, grid_recv,
):
    ins = [
        pltpu.make_async_copy(src, dst, in_sem.at[i])
        for i, (src, dst) in enumerate([
            (owner_hbm, owner_ref), (count_hbm, count_ref), (order_hbm, order_ref), (cell_hbm, cell_ref), (cot_hbm, cot_ref), (obs_hbm, obs_ref),
            (w_in_hbm, w_in_ref), (w_out_hbm, w_out_ref), (bias_hbm, bias_ref), (taps_hbm, taps_ref),
        ])
    ]
    for copy in ins:
        copy.start()

    lat, lon = lax.axis_index("lat"), lax.axis_index("lon")
    z, c, x, y = lax.div(lat, 2), lax.rem(lat, 2), lax.div(lon, 4), lax.rem(lon, 4)
    me = lat * GRP + lon
    up_edge = (lat > 0) & (lon == 0)
    down_edge = (lat < N_GRP - 1) & (lon == GRP - 1)
    zs, cs, xs, ys = ([lax.rem(at + d, n) for d in range(n)] for at, n in ((z, 4), (c, 2), (x, 4), (y, 4)))

    def peer(g, j):
        dz, dc, dx, dy = PLACES[g * GRP + j]
        return zs[dz] * 2 + cs[dc], xs[dx] * 4 + ys[dy]

    plane = [d for d in PLACES if d[:2] == (0, 0)]
    lons = [xs[dx] * 4 + ys[dy] for _, _, dx, dy in plane]

    def members(g):
        return GRP if g < N_GRP - 1 else GRP - 1

    def each_peer(fn):
        for g in range(N_GRP):
            for j in range(members(g)):
                fn(g, j, *peer(g, j))

    def remote(src, dst, send, recv, to_lat, to_lon):
        return pltpu.make_async_remote_copy(
            src_ref=src, dst_ref=dst, send_sem=send, recv_sem=recv,
            device_id=(to_lat, to_lon), device_id_type=MESH,
        )

    def wait_sent(ref, sem):
        remote(ref, ref, sem, sem, lat, lon).wait_send()

    def wait_got(ref, sem):
        remote(ref, ref, sem, sem, lat, lon).wait_recv()


    dep[...] = jnp.zeros_like(dep)
    recv_cot[0] = jnp.zeros(recv_cot.shape[1:], BF16)
    recv_cot[TLAT + 1] = jnp.zeros(recv_cot.shape[1:], BF16)

    barrier = pltpu.get_barrier_semaphore()

    def greet(g, j, to_lat, to_lon):
        pl.semaphore_signal(barrier, inc=1, device_id=(to_lat, to_lon), device_id_type=MESH)

    each_peer(greet)


    for copy in ins[:4]:
        copy.wait()
    owner = owner_ref[...]
    valid = iota((1, OBS), 1) < count_ref[0]
    o_lat, o_lon = owner // GRP, owner % GRP
    dz, dc = (o_lat // 2 - z + 4) % 4, (o_lat - c + 2) % 2
    dx, dy = (o_lon // 4 - x + 4) % 4, (o_lon - y + 4) % 4
    rel = dz * 32 + dc * 16 + dx * 4 + dy
    rel = jnp.where(valid, rel, -1)
    upto = jnp.where(iota((256, 256), 0) <= iota((256, 256), 1), 1.0, 0.0).astype(BF16)
    order = jnp.concatenate([order_ref[...]] * 2, axis=1)
    base = (iota((N_DEV, 256), 0) * CAP).astype(F32)
    carry = jnp.zeros((N_DEV, 1), F32)
    ranks, keys, hits = [], [], []
    for i in range(OBS // 256):
        hit = jnp.where(order == rel[:, i * 256 : (i + 1) * 256], 1.0, 0.0)
        count = mm(hit.astype(BF16), upto) + carry
        ranks.append(jnp.sum(hit * count, axis=0, keepdims=True) - 1.0)
        keys.append(jnp.sum(hit * (count + base), axis=0, keepdims=True) - 1.0)
        carry = count[:, 255:256]
        hits.append(hit)
    rank = jnp.concatenate(ranks, axis=1).astype(I32)
    key = jnp.concatenate(keys, axis=1).astype(I32)


    value = cell_ref[...].reshape(1, OBS) + 1
    high = jnp.where(value >= 256, 1.0, 0.0)
    low = value.astype(F32) - 256.0 * high
    cells_high = jnp.zeros((N_DEV, 128), F32)
    cells_low = jnp.zeros((N_DEV, 128), F32)
    for i in range(OBS // 256):
        part = slice(i * 256, (i + 1) * 256)
        hit = hits[i]
        place = jnp.where(iota((128, 256), 0) == rank[:, part], 1.0, 0.0).astype(BF16)
        cells_high += mm_nt((hit * high[:, part]).astype(BF16), place)
        cells_low += mm_nt((hit * low[:, part]).astype(BF16), place)
    cells = (256.0 * cells_high + cells_low).reshape(N_GRP, GRP, 128)
    send_cells[...] = cells
    recv_cells[N_GRP - 1, GRP - 1 :] = cells[N_GRP - 1, GRP - 1 :]


    ins[4].wait()
    where_from = iota((GRP * 32, GLON), 0)
    tile, slot = where_from // 32, where_from % 32
    column = jnp.where(
        slot < TLON,
        tile * TLON + slot,
        jnp.where(
            slot == TLON,
            (tile * TLON + GLON - 1) % GLON,
            jnp.where(slot == TLON + 1, (tile * TLON + TLON) % GLON, -1),
        ),
    )
    pick = jnp.where(column == iota((GRP * 32, GLON), 1), 1.0, 0.0).astype(BF16)
    send_cot[...] = mm(pick, cot_ref[...]).reshape(GRP, 32, CH)[:, :26].astype(BF16)
    recv_cot[1 + lon] = send_cot[lon]


    ins[5].wait()

    def pack(g):
        total = jnp.zeros((SLOTS, FEAT), F32)
        for i in range(OBS // 256):
            part = slice(i * 256, (i + 1) * 256)
            take = jnp.where(iota((SLOTS, 256), 0) + g * SLOTS == key[:, part], 1.0, 0.0)
            total += mm(take.astype(BF16), obs_ref[part, :])
        send_rows[g * GRP : (g + 1) * GRP] = total.reshape(GRP, CAP, FEAT).astype(BF16)

    def send_group(g):
        for j in range(members(g)):
            remote(
                send_rows.at[g * GRP + j], recv_rows.at[g * GRP + j],
                row_send.at[g], row_recv.at[g], *peer(g, j),
            ).start()

    for g in range(EARLY):
        pack(g)


    pl.semaphore_wait(barrier, N_DEV - 1)


    def send_cell(g, j, to_lat, to_lon):
        remote(
            send_cells.at[g, pl.ds(j, 1)], recv_cells.at[g, pl.ds(j, 1)],
            cell_send.at[g], cell_recv.at[g], to_lat, to_lon,
        ).start()

    each_peer(send_cell)
    for j in range(GRP - 1):
        remote(
            send_cot.at[lons[j]], recv_cot.at[1 + lon], cot_send, cot_recv, lat, lons[j]
        ).start()

    @pl.when(up_edge)
    def _():
        for j in range(GRP):
            remote(
                send_cot.at[lons[j]], recv_cot.at[TLAT + 1], edge_send.at[0], edge_recv.at[0],
                lat - 1, lons[j],
            ).start()

    @pl.when(down_edge)
    def _():
        for j in range(GRP):
            remote(
                send_cot.at[lons[j]], recv_cot.at[0], edge_send.at[1], edge_recv.at[1],
                lat + 1, lons[j],
            ).start()


    for g in range(EARLY, HOLD):
        pack(g)
    for g in range(HOLD):
        send_group(g)
    for g in range(HOLD, N_GRP):
        pack(g)
        send_group(g)
    recv_rows[N_DEV - 1] = send_rows[N_DEV - 1]


    for copy in ins[6:]:
        copy.wait()
    w_in_t = w_in_ref[...].astype(F32).T.astype(BF16)
    w_out = w_out_ref[...]
    w_out_t = w_out.astype(F32).T.astype(BF16)
    bias_t = jnp.broadcast_to(bias_ref[...], (128, HID)).T[:, 0:1]
    for g in range(N_GRP):
        wait_got(recv_cells.at[g, pl.ds(0, members(g))], cell_recv.at[g])
    codes = recv_cells[...].reshape(N_DEV, 128)
    high = jnp.where(codes >= 256.0, 1.0, 0.0)
    spread = jnp.where(iota((128, SLOTS), 0) == iota((128, SLOTS), 1) % CAP, 1.0, 0.0).astype(BF16)
    codes = 256.0 * mm(high.astype(BF16), spread) + mm((codes - 256.0 * high).astype(BF16), spread)
    own = iota((GRP, SLOTS), 0) == iota((GRP, SLOTS), 1) // CAP

    for g in range(N_GRP):
        mine = jnp.where(own, codes[g * GRP : (g + 1) * GRP], 0.0)
        cell_of = jnp.sum(mine, axis=0, keepdims=True).astype(I32) - 1
        hit = jnp.where(iota((CELLS, SLOTS), 0) == cell_of, 1.0, 0.0)
        places[:, g * SLOTS : (g + 1) * SLOTS] = hit.astype(BF16)


    wait_got(recv_cot.at[pl.ds(0, GRP - 1)], cot_recv)


    def spread_cot(rows):
        part = recv_cot[rows].astype(F32)
        cot_f[rows, 8:32, :] = part[:, 0:TLON]
        cot_f[rows, 7:8, :] = part[:, TLON : TLON + 1]
        cot_f[rows, 32:33, :] = part[:, TLON + 1 : TLON + 2]
        for b in (-1, 0, 1):
            cot_s[b + 1, rows] = cot_f[rows, 8 - b : 8 - b + TLON, :]

    def adjoint_row(r, carry):
        total = jnp.zeros((TLON, CH), F32)
        for k, (a, b) in enumerate(TAPS):
            total += taps_ref[k : k + 1, :] * cot_s[b + 1, r + 1 - a]
        send_grid[r] = (SCALE * total).astype(BF16)
        return carry

    spread_cot(slice(1, TLAT + 1))
    lax.fori_loop(1, TLAT - 1, adjoint_row, 0)


    @pl.when(lat < N_GRP - 1)
    def _():
        wait_got(recv_cot.at[TLAT + 1], edge_recv.at[0])

    @pl.when(lat > 0)
    def _():
        wait_got(recv_cot.at[0], edge_recv.at[1])


    for row in (0, TLAT + 1):
        spread_cot(slice(row, row + 1))
    adjoint_row(0, 0)
    adjoint_row(TLAT - 1, 0)
    adj_t[...] = send_grid[...].astype(F32).reshape(CELLS, CH).T.astype(BF16)


    for i in range(0, N_GRP, 4):
        at = slice(i * SLOTS, (i + 4) * SLOTS)
        up = mm(adj_t[...], places[:, at]).astype(BF16)
        ups[:, at] = up
        backs[:, at] = mm(w_out, up)

    acc_in[...] = jnp.zeros_like(acc_in)
    acc_out[...] = jnp.zeros_like(acc_out)

    def work(groups):
        start, count = groups[0], len(groups)
        at = slice(start * SLOTS, (start + count) * SLOTS)
        rows = recv_rows[start * GRP : (start + count) * GRP]
        rows = rows.astype(F32).reshape(count * SLOTS, FEAT).astype(BF16)
        before = mm_nt(w_in_t, rows) + bias_t
        square = before * before
        half = 0.5 + 0.5 * jnp.tanh(before * (C0 + C0 * C1 * square))
        value = before * half
        hidden = value.astype(BF16)
        slope = half + value * (1.0 - half) * (2.0 * C0 + 6.0 * C0 * C1 * square)
        pre = (backs[:, at] * slope).astype(BF16)
        encoded = mm(w_out_t, hidden).astype(BF16)
        add = mm_nt(places[:, at], encoded).reshape(TLAT, TLON, CH)
        dep[1 : 1 + TLAT, 8 : 8 + TLON, :] += add
        acc_out[...] += mm_nt(hidden, ups[:, at])
        ones = jnp.ones((count * SLOTS, 128), BF16)
        acc_in[...] += mm(pre, jnp.concatenate([rows, ones], axis=1))

    for groups in STEPS:

        for g in groups:
            wait_got(recv_rows.at[pl.ds(g * GRP, members(g))], row_recv.at[g])

        work(groups)


    north, south = lat > 0, lat < N_GRP - 1
    west, east = lax.rem(lon + 15, GRP), lax.rem(lon + 1, GRP)
    core = (1, TLAT)
    first, last = (1, 1), (TLAT, 1)
    above, below = (0, 1), (TLAT + 1, 1)
    wide, left, right = (8, TLON), (8, 1), (8 + TLON - 1, 1)
    before_left, after_right = (7, 1), (8 + TLON, 1)
    halos = [
        (None, lat, west, core, left, core, after_right),
        (None, lat, east, core, right, core, before_left),
        (north, lat - 1, lon, first, wide, below, wide),
        (south, lat + 1, lon, last, wide, above, wide),
        (north, lat - 1, west, first, left, below, after_right),
        (north, lat - 1, east, first, right, below, before_left),
        (south, lat + 1, west, last, left, above, after_right),
        (south, lat + 1, east, last, right, above, before_left),
    ]
    comes = [None, None, south, north, south, south, north, north]

    def at(rows, columns):
        return dep.at[pl.ds(*rows), pl.ds(*columns), :]

    for i, (there, to_lat, to_lon, sr, sc, dr, dc) in enumerate(halos):
        def send_halo(i=i, to_lat=to_lat, to_lon=to_lon, sr=sr, sc=sc, dr=dr, dc=dc):
            remote(
                at(sr, sc), at(dr, dc), halo_send.at[i], halo_recv.at[i], to_lat, to_lon
            ).start()

        send_halo() if there is None else pl.when(there)(send_halo)


    def taps_row(r, totals):
        for at in range(0, TLON, 8):
            mine = dep[r + 1, 8 + at : 16 + at, :]
            totals = tuple(
                total + mine * cot_s[b + 1, r + 1 - a, at : at + 8]
                for total, (a, b) in zip(totals, TAPS)
            )
        return totals

    totals = lax.fori_loop(0, TLAT, taps_row, (jnp.zeros((8, CH), F32),) * 9)
    small = [SCALE * jnp.sum(t, axis=0, keepdims=True) for t in totals]
    small.append(acc_in[:, FEAT:].T[0:1])
    small = [h for s in small for h in (s[:, :128], s[:, 128:])]
    small = jnp.concatenate(small + [jnp.zeros((4, 128), F32)], axis=0)
    small_high = small.astype(BF16)
    small_low = (small - small_high.astype(F32)).astype(BF16)

    chunks[0:32] = acc_in[:, :FEAT].reshape(32, 8, 128).astype(BF16)
    chunks[32:64] = acc_out[:, :128].reshape(32, 8, 128).astype(BF16)
    chunks[64:96] = acc_out[:, 128:].reshape(32, 8, 128).astype(BF16)
    chunks[96:99] = small_high.astype(F32).reshape(3, 8, 128).astype(BF16)
    chunks[99:102] = small_low.astype(F32).reshape(3, 8, 128).astype(BF16)
    chunks[102:128] = jnp.zeros((26, 8, 128), BF16)

    def send_part(g, j, to_lat, to_lon):
        remote(
            chunks.at[to_lat * GRP + to_lon], parts.at[g * GRP + j],
            part_send.at[g], part_recv.at[g], to_lat, to_lon,
        ).start()


    each_peer(send_part)
    parts[N_DEV - 1] = chunks[me]


    for i, there in enumerate(comes):
        _, _, _, _, _, dr, dc = halos[i]
        def got_halo(i=i, dr=dr, dc=dc):
            wait_got(at(dr, dc), halo_recv.at[i])

        got_halo() if there is None else pl.when(there)(got_halo)


    def grid_row(r, carry):
        total = jnp.zeros((TLON, CH), F32)
        for k, (a, b) in enumerate(TAPS):
            total += taps_ref[k : k + 1, :] * dep[r + 1 + a, 8 + b : 8 + b + TLON, :]
        send_grid[r] = total.astype(BF16)
        return carry

    lax.fori_loop(0, TLAT, grid_row, 0)
    for j in range(GRP - 1):
        remote(
            send_grid.at[lons[j]], grid_ref.at[lon], grid_send, grid_recv, lat, lons[j]
        ).start()
    mine_grid = pltpu.make_async_copy(send_grid.at[lon], grid_ref.at[lon], own_sem.at[0])
    mine_grid.start()


    for g in range(N_GRP):
        wait_got(parts.at[pl.ds(g * GRP, members(g))], part_recv.at[g])

    mine = jnp.sum(parts[...].astype(F32), axis=0).astype(BF16)
    red[...] = mine
    mine_share = pltpu.make_async_copy(red, shared.at[me], own_sem.at[1])
    mine_share.start()

    def send_share(g, j, to_lat, to_lon):
        remote(
            red, shared.at[me], share_send.at[g], share_recv.at[g], to_lat, to_lon
        ).start()


    each_peer(send_share)


    for g in range(N_GRP):
        wait_got(shared.at[pl.ds(g * GRP, members(g))], share_recv.at[g])

    mine_grid.wait()
    mine_share.wait()
    wait_got(grid_ref.at[pl.ds(0, GRP - 1)], grid_recv)
    for g in range(N_GRP):
        n = members(g)
        wait_sent(send_cells.at[g, pl.ds(0, n)], cell_send.at[g])
        wait_sent(send_rows.at[pl.ds(g * GRP, n)], row_send.at[g])
        wait_sent(chunks.at[pl.ds(g * GRP, n)], part_send.at[g])
        wait_sent(shared.at[pl.ds(g * GRP, n)], share_send.at[g])
    wait_sent(send_cot.at[pl.ds(0, GRP - 1)], cot_send)
    wait_sent(send_grid.at[pl.ds(0, GRP - 1)], grid_send)

    @pl.when(up_edge)
    def _():
        wait_sent(send_cot, edge_send.at[0])

    @pl.when(down_edge)
    def _():
        wait_sent(send_cot, edge_send.at[1])

    for i, (there, _, _, sr, sc, _, _) in enumerate(halos):
        def sent_halo(i=i, sr=sr, sc=sc):
            wait_sent(at(sr, sc), halo_send.at[i])

        sent_halo() if there is None else pl.when(there)(sent_halo)


def finish(
    grid_in, shared_in, grid_hbm, g_in_hbm, g_bias_hbm, g_out_hbm, g_taps_hbm,
    grid, shared, g_in, g_bias, g_out, g_taps, sem,
):
    come = pltpu.make_async_copy(shared_in, shared, sem.at[5])
    come.start()
    grid_come = pltpu.make_async_copy(grid_in, grid, sem.at[6])
    grid_come.start()
    copies = [pltpu.make_async_copy(grid, grid_hbm, sem.at[0])]
    come.wait()
    g_out[:, :128] = shared[32:64].astype(F32).reshape(HID, 128)
    g_out[:, 128:] = shared[64:96].astype(F32).reshape(HID, 128)
    copies.append(pltpu.make_async_copy(g_out, g_out_hbm, sem.at[1]))
    copies[1].start()
    g_in[...] = shared[0:32].astype(F32).reshape(HID, FEAT).T
    copies.append(pltpu.make_async_copy(g_in, g_in_hbm, sem.at[2]))
    copies[2].start()
    grid_come.wait()
    copies[0].start()
    small = (shared[96:99].astype(F32) + shared[99:102].astype(F32)).reshape(24, 128)
    for k in range(9):
        g_taps[k : k + 1, :128] = small[2 * k : 2 * k + 1]
        g_taps[k : k + 1, 128:] = small[2 * k + 1 : 2 * k + 2]
    g_bias[:, :128] = small[18:19]
    g_bias[:, 128:] = small[19:20]
    copies.append(pltpu.make_async_copy(g_taps, g_taps_hbm, sem.at[3]))
    copies.append(pltpu.make_async_copy(g_bias, g_bias_hbm, sem.at[4]))
    copies[3].start()
    copies[4].start()
    for copy in copies:
        copy.wait()


def local(obs, owner, cell, count, w_in, bias, w_out, taps, cot):
    hbm = pl.BlockSpec(memory_space=pltpu.HBM)
    dma = pltpu.SemaphoreType.DMA
    order = [dz * 32 + dc * 16 + dx * 4 + dy for dz, dc, dx, dy in PLACES]
    order = jnp.asarray(np.repeat(np.array(order, np.int32)[:, None], 128, axis=1))
    rows, shared = pl.pallas_call(
        kernel,
        name="encode_step",
        out_shape=(
            jax.ShapeDtypeStruct((GRP, TLON, CH), BF16),
            jax.ShapeDtypeStruct((N_DEV, 8, 128), BF16),
        ),
        in_specs=[hbm] * 10,
        out_specs=(hbm,) * 2,
        scratch_shapes=[
            pltpu.VMEM((OBS, FEAT), BF16),
            pltpu.VMEM((1, OBS), I32),
            pltpu.VMEM((OBS,), I32),
            pltpu.SMEM((1,), I32),
            pltpu.VMEM((N_DEV, 128), I32),
            pltpu.VMEM((FEAT, HID), BF16),
            pltpu.VMEM((1, HID), F32),
            pltpu.VMEM((HID, CH), BF16),
            pltpu.VMEM((9, CH), F32),
            pltpu.VMEM((GLON, CH), BF16),
            pltpu.VMEM((N_DEV, CAP, FEAT), BF16),
            pltpu.VMEM((N_DEV, CAP, FEAT), BF16),
            pltpu.VMEM((N_GRP, GRP, 128), F32),
            pltpu.VMEM((N_GRP, GRP, 128), F32),
            pltpu.VMEM((GRP, 26, CH), BF16),
            pltpu.VMEM((TLAT + 2, 26, CH), BF16),
            pltpu.VMEM((TLAT + 2, 40, CH), F32),
            pltpu.VMEM((3, TLAT + 2, TLON, CH), F32),
            pltpu.VMEM((TLAT + 2, 40, CH), F32),
            pltpu.VMEM((TLAT, TLON, CH), BF16),
            pltpu.VMEM((N_DEV, 8, 128), BF16),
            pltpu.VMEM((N_DEV, 8, 128), BF16),
            pltpu.VMEM((8, 128), BF16),
            pltpu.VMEM((HID, 2 * FEAT), F32),
            pltpu.VMEM((HID, CH), F32),
            pltpu.VMEM((CH, CELLS), BF16),
            pltpu.VMEM((CELLS, N_GRP * SLOTS), BF16),
            pltpu.VMEM((CH, N_GRP * SLOTS), BF16),
            pltpu.VMEM((HID, N_GRP * SLOTS), F32),
            dma((10,)), dma((2,)),
            dma((N_GRP,)), dma((N_GRP,)), dma((N_GRP,)), dma((N_GRP,)),
            dma, dma, dma((2,)), dma((2,)),
            dma((N_GRP,)), dma((N_GRP,)), dma((N_GRP,)), dma((N_GRP,)),
            dma((8,)), dma((8,)), dma, dma,
        ],
        compiler_params=pltpu.CompilerParams(
            collective_id=0, has_side_effects=True, vmem_limit_bytes=67043328
        ),
        cost_estimate=pl.CostEstimate(
            flops=4_000_000_000, bytes_accessed=2_000_000, transcendentals=800_000
        ),
    )(
        obs, owner.reshape(1, OBS), cell, count, order, w_in, bias.reshape(1, HID),
        w_out, taps, cot.reshape(GLON, CH),
    )
    outs = [((GRP, TLON, CH), BF16), ((FEAT, HID), F32), ((1, HID), F32), ((HID, CH), F32), ((9, CH), F32)]
    grid, g_in, g_bias, g_out, g_taps = pl.pallas_call(
        finish,
        name="finish",
        out_shape=tuple(jax.ShapeDtypeStruct(*o) for o in outs),
        in_specs=[hbm, hbm],
        out_specs=(hbm,) * 5,
        scratch_shapes=[
            pltpu.VMEM(*outs[0]),
            pltpu.VMEM((N_DEV, 8, 128), BF16),
            *[pltpu.VMEM(*o) for o in outs[1:]],
            dma((7,)),
        ],
        compiler_params=pltpu.CompilerParams(vmem_limit_bytes=67043328),
    )(rows, shared)
    return (grid.reshape(1, GLON, CH), g_in, g_bias.reshape(HID), g_out, g_taps)


def solution(mesh):
    block = P(("lat", "lon"))
    return jax.shard_map(
        local,
        mesh=mesh,
        in_specs=(block, block, block, block, P(), P(), P(), P(), block),
        out_specs=(block, P(), P(), P(), P()),
        check_vma=False,
    )
```

```python
import functools
import math

import jax
import jax.numpy as jnp
import numpy as np
from jax import lax
from jax.experimental import pallas as pl
from jax.experimental.pallas import tpu as pltpu
from jax.sharding import PartitionSpec as P

MESH = pl.DeviceIdType.MESH
F32, BF16, I32 = jnp.float32, jnp.bfloat16, jnp.int32
NT = (((1,), (1,)), ((), ()))
TAPS = [(a, b) for a in (-1, 0, 1) for b in (-1, 0, 1)]

N_DEV, N_GRP, GRP = 128, 8, 16
EARLY = 3
HOLD = 8
STEPS = ((0, 1), (2, 3), (4, 5, 6, 7))
OBS, FEAT, HID, CH = 1536, 128, 256, 256
CAP = 24
SLOTS = GRP * CAP
TLAT, TLON = 16, 24
CELLS = TLAT * TLON
GLON = 384
CHUNKS_IN, CHUNKS_OUT, CHUNKS_SMALL = 32, 64, 3
SCALE = 1.0 / math.sqrt(OBS * N_DEV)
C0, C1 = math.sqrt(2.0 / math.pi), 0.044715


def iota(shape, dim):
    return lax.broadcasted_iota(I32, shape, dim)


def mm(a, b):
    return jnp.dot(a, b, preferred_element_type=F32)


def mm_nt(a, b):
    return lax.dot_general(a, b, NT, preferred_element_type=F32)


def hops(offset):
    dz, dc, dx, dy = offset
    return sum(min(d, 4 - d) for d in (dz, dx, dy)) + 0.1 * dc


PLACES = sorted(
    ((i // 32, i // 16 % 2, i // 4 % 4, i % 4) for i in range(N_DEV)), key=hops, reverse=True
)


def kernel(
    obs_hbm, owner_hbm, cell_hbm, count_hbm, order_hbm, w_in_hbm, bias_hbm, w_out_hbm, taps_hbm, cot_hbm,
    grid_ref, shared,
    obs_ref, owner_ref, cell_ref, count_ref, order_ref, w_in_ref, bias_ref, w_out_ref, taps_ref, cot_ref,
    send_rows, recv_rows, send_cells, recv_cells, send_cot, recv_cot, cot_f, cot_s, dep, send_grid,
    chunks, parts, red, acc_in, acc_out, adj_t, places, ups, backs,
    in_sem, own_sem,
    row_send, row_recv, cell_send, cell_recv, cot_send, cot_recv, edge_send, edge_recv,
    part_send, part_recv, share_send, share_recv, halo_send, halo_recv, grid_send, grid_recv,
):
    ins = [
        pltpu.make_async_copy(src, dst, in_sem.at[i])
        for i, (src, dst) in enumerate([
            (owner_hbm, owner_ref), (count_hbm, count_ref), (order_hbm, order_ref), (cell_hbm, cell_ref), (cot_hbm, cot_ref), (obs_hbm, obs_ref),
            (w_in_hbm, w_in_ref), (w_out_hbm, w_out_ref), (bias_hbm, bias_ref), (taps_hbm, taps_ref),
        ])
    ]
    for copy in ins:
        copy.start()

    lat, lon = lax.axis_index("lat"), lax.axis_index("lon")
    z, c, x, y = lax.div(lat, 2), lax.rem(lat, 2), lax.div(lon, 4), lax.rem(lon, 4)
    me = lat * GRP + lon
    up_edge = (lat > 0) & (lon == 0)
    down_edge = (lat < N_GRP - 1) & (lon == GRP - 1)
    zs, cs, xs, ys = ([lax.rem(at + d, n) for d in range(n)] for at, n in ((z, 4), (c, 2), (x, 4), (y, 4)))

    def peer(g, j):
        dz, dc, dx, dy = PLACES[g * GRP + j]
        return zs[dz] * 2 + cs[dc], xs[dx] * 4 + ys[dy]

    plane = [d for d in PLACES if d[:2] == (0, 0)]
    lons = [xs[dx] * 4 + ys[dy] for _, _, dx, dy in plane]

    def members(g):
        return GRP if g < N_GRP - 1 else GRP - 1

    def each_peer(fn):
        for g in range(N_GRP):
            for j in range(members(g)):
                fn(g, j, *peer(g, j))

    def remote(src, dst, send, recv, to_lat, to_lon):
        return pltpu.make_async_remote_copy(
            src_ref=src, dst_ref=dst, send_sem=send, recv_sem=recv,
            device_id=(to_lat, to_lon), device_id_type=MESH,
        )

    def wait_sent(ref, sem):
        remote(ref, ref, sem, sem, lat, lon).wait_send()

    def wait_got(ref, sem):
        remote(ref, ref, sem, sem, lat, lon).wait_recv()


    dep[0:1] = jnp.zeros((1, 40, CH), F32)
    dep[TLAT + 1 :] = jnp.zeros((1, 40, CH), F32)
    recv_cot[0] = jnp.zeros(recv_cot.shape[1:], BF16)
    recv_cot[TLAT + 1] = jnp.zeros(recv_cot.shape[1:], BF16)

    barrier = pltpu.get_barrier_semaphore()

    def greet(g, j, to_lat, to_lon):
        pl.semaphore_signal(barrier, inc=1, device_id=(to_lat, to_lon), device_id_type=MESH)

    each_peer(greet)
    dep[1 : 1 + TLAT, 8 : 8 + TLON, :] = jnp.zeros((TLAT, TLON, CH), F32)


    for copy in ins[:4]:
        copy.wait()
    owner = owner_ref[...]
    valid = iota((1, OBS), 1) < count_ref[0]
    o_lat, o_lon = owner // GRP, owner % GRP
    dz, dc = (o_lat // 2 - z + 4) % 4, (o_lat - c + 2) % 2
    dx, dy = (o_lon // 4 - x + 4) % 4, (o_lon - y + 4) % 4
    rel = dz * 32 + dc * 16 + dx * 4 + dy
    rel = jnp.where(valid, rel, -1)
    upto = jnp.where(iota((256, 256), 0) <= iota((256, 256), 1), 1.0, 0.0).astype(BF16)
    order = jnp.concatenate([order_ref[...]] * 2, axis=1)
    base = (iota((N_DEV, 256), 0) * CAP).astype(F32)
    carry = jnp.zeros((N_DEV, 1), F32)
    ranks, keys, hits = [], [], []
    for i in range(OBS // 256):
        hit = jnp.where(order == rel[:, i * 256 : (i + 1) * 256], 1.0, 0.0)
        count = mm(hit.astype(BF16), upto) + carry
        ranks.append(jnp.sum(hit * count, axis=0, keepdims=True) - 1.0)
        keys.append(jnp.sum(hit * (count + base), axis=0, keepdims=True) - 1.0)
        carry = count[:, 255:256]
        hits.append(hit)
    rank = jnp.concatenate(ranks, axis=1).astype(I32)
    key = jnp.concatenate(keys, axis=1).astype(I32)


    value = cell_ref[...].reshape(1, OBS) + 1
    high = jnp.where(value >= 256, 1.0, 0.0)
    low = value.astype(F32) - 256.0 * high
    cells_high = jnp.zeros((N_DEV, 128), F32)
    cells_low = jnp.zeros((N_DEV, 128), F32)
    for i in range(OBS // 256):
        part = slice(i * 256, (i + 1) * 256)
        hit = hits[i]
        place = jnp.where(iota((128, 256), 0) == rank[:, part], 1.0, 0.0).astype(BF16)
        cells_high += mm_nt((hit * high[:, part]).astype(BF16), place)
        cells_low += mm_nt((hit * low[:, part]).astype(BF16), place)
    cells = (256.0 * cells_high + cells_low).reshape(N_GRP, GRP, 128)
    send_cells[...] = cells
    recv_cells[N_GRP - 1, GRP - 1 :] = cells[N_GRP - 1, GRP - 1 :]


    ins[4].wait()
    where_from = iota((GRP * 32, GLON), 0)
    tile, slot = where_from // 32, where_from % 32
    column = jnp.where(
        slot < TLON,
        tile * TLON + slot,
        jnp.where(
            slot == TLON,
            (tile * TLON + GLON - 1) % GLON,
            jnp.where(slot == TLON + 1, (tile * TLON + TLON) % GLON, -1),
        ),
    )
    pick = jnp.where(column == iota((GRP * 32, GLON), 1), 1.0, 0.0).astype(BF16)
    send_cot[...] = mm(pick, cot_ref[...]).reshape(GRP, 32, CH)[:, :26].astype(BF16)
    recv_cot[1 + lon] = send_cot[lon]


    ins[5].wait()

    def pack(g):
        total = jnp.zeros((SLOTS, FEAT), F32)
        for i in range(OBS // 256):
            part = slice(i * 256, (i + 1) * 256)
            take = jnp.where(iota((SLOTS, 256), 0) + g * SLOTS == key[:, part], 1.0, 0.0)
            total += mm(take.astype(BF16), obs_ref[part, :])
        send_rows[g * GRP : (g + 1) * GRP] = total.reshape(GRP, CAP, FEAT).astype(BF16)

    def send_group(g):
        for j in range(members(g)):
            remote(
                send_rows.at[g * GRP + j], recv_rows.at[g * GRP + j],
                row_send.at[g], row_recv.at[g], *peer(g, j),
            ).start()

    for g in range(EARLY):
        pack(g)


    pl.semaphore_wait(barrier, N_DEV - 1)


    def send_cell(g, j, to_lat, to_lon):
        remote(
            send_cells.at[g, pl.ds(j, 1)], recv_cells.at[g, pl.ds(j, 1)],
            cell_send.at[g], cell_recv.at[g], to_lat, to_lon,
        ).start()

    each_peer(send_cell)
    for j in range(GRP - 1):
        remote(
            send_cot.at[lons[j]], recv_cot.at[1 + lon], cot_send, cot_recv, lat, lons[j]
        ).start()

    @pl.when(up_edge)
    def _():
        for j in range(GRP):
            remote(
                send_cot.at[lons[j]], recv_cot.at[TLAT + 1], edge_send.at[0], edge_recv.at[0],
                lat - 1, lons[j],
            ).start()

    @pl.when(down_edge)
    def _():
        for j in range(GRP):
            remote(
                send_cot.at[lons[j]], recv_cot.at[0], edge_send.at[1], edge_recv.at[1],
                lat + 1, lons[j],
            ).start()


    for g in range(EARLY, HOLD):
        pack(g)
    for g in range(HOLD):
        send_group(g)
    for g in range(HOLD, N_GRP):
        pack(g)
        send_group(g)
    recv_rows[N_DEV - 1] = send_rows[N_DEV - 1]


    for copy in ins[6:]:
        copy.wait()
    w_in_t = w_in_ref[...].astype(F32).T.astype(BF16)
    w_out = w_out_ref[...]
    w_out_t = w_out.astype(F32).T.astype(BF16)
    bias_t = jnp.broadcast_to(bias_ref[...], (128, HID)).T[:, 0:1]
    for g in range(N_GRP):
        wait_got(recv_cells.at[g, pl.ds(0, members(g))], cell_recv.at[g])
    codes = recv_cells[...].reshape(N_DEV, 128)
    high = jnp.where(codes >= 256.0, 1.0, 0.0)
    spread = jnp.where(iota((128, SLOTS), 0) == iota((128, SLOTS), 1) % CAP, 1.0, 0.0).astype(BF16)
    codes = 256.0 * mm(high.astype(BF16), spread) + mm((codes - 256.0 * high).astype(BF16), spread)
    own = iota((GRP, SLOTS), 0) == iota((GRP, SLOTS), 1) // CAP

    for g in range(N_GRP):
        mine = jnp.where(own, codes[g * GRP : (g + 1) * GRP], 0.0)
        cell_of = jnp.sum(mine, axis=0, keepdims=True).astype(I32) - 1
        hit = jnp.where(iota((CELLS, SLOTS), 0) == cell_of, 1.0, 0.0)
        places[:, g * SLOTS : (g + 1) * SLOTS] = hit.astype(BF16)


    wait_got(recv_cot.at[pl.ds(0, GRP - 1)], cot_recv)


    def spread_cot(rows):
        part = recv_cot[rows].astype(F32)
        cot_f[rows, 8:32, :] = part[:, 0:TLON]
        cot_f[rows, 7:8, :] = part[:, TLON : TLON + 1]
        cot_f[rows, 32:33, :] = part[:, TLON + 1 : TLON + 2]
        for b in (-1, 0, 1):
            cot_s[b + 1, rows] = cot_f[rows, 8 - b : 8 - b + TLON, :]

    def adjoint_row(r, carry):
        total = jnp.zeros((TLON, CH), F32)
        for k, (a, b) in enumerate(TAPS):
            total += taps_ref[k : k + 1, :] * cot_s[b + 1, r + 1 - a]
        send_grid[r] = (SCALE * total).astype(BF16)
        return carry

    spread_cot(slice(1, TLAT + 1))
    lax.fori_loop(1, TLAT - 1, adjoint_row, 0)


    @pl.when(lat < N_GRP - 1)
    def _():
        wait_got(recv_cot.at[TLAT + 1], edge_recv.at[0])

    @pl.when(lat > 0)
    def _():
        wait_got(recv_cot.at[0], edge_recv.at[1])


    for row in (0, TLAT + 1):
        spread_cot(slice(row, row + 1))
    adjoint_row(0, 0)
    adjoint_row(TLAT - 1, 0)
    adj_t[...] = send_grid[...].astype(F32).reshape(CELLS, CH).T.astype(BF16)


    for i in range(0, N_GRP, 4):
        at = slice(i * SLOTS, (i + 4) * SLOTS)
        up = mm(adj_t[...], places[:, at]).astype(BF16)
        ups[:, at] = up
        backs[:, at] = mm(w_out, up)

    acc_in[...] = jnp.zeros_like(acc_in)
    acc_out[...] = jnp.zeros_like(acc_out)

    def work(groups):
        start, count = groups[0], len(groups)
        at = slice(start * SLOTS, (start + count) * SLOTS)
        rows = recv_rows[start * GRP : (start + count) * GRP]
        rows = rows.astype(F32).reshape(count * SLOTS, FEAT).astype(BF16)
        before = mm_nt(w_in_t, rows) + bias_t
        square = before * before
        half = 0.5 + 0.5 * jnp.tanh(before * (C0 + C0 * C1 * square))
        value = before * half
        hidden = value.astype(BF16)
        slope = half + value * (1.0 - half) * (2.0 * C0 + 6.0 * C0 * C1 * square)
        pre = (backs[:, at] * slope).astype(BF16)
        encoded = mm(w_out_t, hidden).astype(BF16)
        add = mm_nt(places[:, at], encoded).reshape(TLAT, TLON, CH)
        dep[1 : 1 + TLAT, 8 : 8 + TLON, :] += add
        acc_out[...] += mm_nt(hidden, ups[:, at])
        ones = jnp.ones((count * SLOTS, 128), BF16)
        acc_in[...] += mm(pre, jnp.concatenate([rows, ones], axis=1))

    for groups in STEPS:

        for g in groups:
            wait_got(recv_rows.at[pl.ds(g * GRP, members(g))], row_recv.at[g])

        work(groups)


    north, south = lat > 0, lat < N_GRP - 1
    west, east = lax.rem(lon + 15, GRP), lax.rem(lon + 1, GRP)
    core = (1, TLAT)
    first, last = (1, 1), (TLAT, 1)
    above, below = (0, 1), (TLAT + 1, 1)
    wide, left, right = (8, TLON), (8, 1), (8 + TLON - 1, 1)
    before_left, after_right = (7, 1), (8 + TLON, 1)
    halos = [
        (None, lat, west, core, left, core, after_right),
        (None, lat, east, core, right, core, before_left),
        (north, lat - 1, lon, first, wide, below, wide),
        (south, lat + 1, lon, last, wide, above, wide),
        (north, lat - 1, west, first, left, below, after_right),
        (north, lat - 1, east, first, right, below, before_left),
        (south, lat + 1, west, last, left, above, after_right),
        (south, lat + 1, east, last, right, above, before_left),
    ]
    comes = [None, None, south, north, south, south, north, north]

    def at(rows, columns):
        return dep.at[pl.ds(*rows), pl.ds(*columns), :]

    for i, (there, to_lat, to_lon, sr, sc, dr, dc) in enumerate(halos):
        def send_halo(i=i, to_lat=to_lat, to_lon=to_lon, sr=sr, sc=sc, dr=dr, dc=dc):
            remote(
                at(sr, sc), at(dr, dc), halo_send.at[i], halo_recv.at[i], to_lat, to_lon
            ).start()

        send_halo() if there is None else pl.when(there)(send_halo)


    def taps_row(r, totals):
        for at in range(0, TLON, 8):
            mine = dep[r + 1, 8 + at : 16 + at, :]
            totals = tuple(
                total + mine * cot_s[b + 1, r + 1 - a, at : at + 8]
                for total, (a, b) in zip(totals, TAPS)
            )
        return totals

    totals = lax.fori_loop(0, TLAT, taps_row, (jnp.zeros((8, CH), F32),) * 9)
    small = [SCALE * jnp.sum(t, axis=0, keepdims=True) for t in totals]
    small.append(acc_in[:, FEAT:].T[0:1])
    small = [h for s in small for h in (s[:, :128], s[:, 128:])]
    small = jnp.concatenate(small + [jnp.zeros((4, 128), F32)], axis=0)
    small_high = small.astype(BF16)
    small_low = (small - small_high.astype(F32)).astype(BF16)

    chunks[0:32] = acc_in[:, :FEAT].reshape(32, 8, 128).astype(BF16)
    chunks[32:64] = acc_out[:, :128].reshape(32, 8, 128).astype(BF16)
    chunks[64:96] = acc_out[:, 128:].reshape(32, 8, 128).astype(BF16)
    chunks[96:99] = small_high.astype(F32).reshape(3, 8, 128).astype(BF16)
    chunks[99:102] = small_low.astype(F32).reshape(3, 8, 128).astype(BF16)
    chunks[102:128] = jnp.zeros((26, 8, 128), BF16)

    def send_part(g, j, to_lat, to_lon):
        remote(
            chunks.at[to_lat * GRP + to_lon], parts.at[g * GRP + j],
            part_send.at[g], part_recv.at[g], to_lat, to_lon,
        ).start()


    each_peer(send_part)
    parts[N_DEV - 1] = chunks[me]


    for i, there in enumerate(comes):
        _, _, _, _, _, dr, dc = halos[i]
        def got_halo(i=i, dr=dr, dc=dc):
            wait_got(at(dr, dc), halo_recv.at[i])

        got_halo() if there is None else pl.when(there)(got_halo)


    def grid_row(r, carry):
        total = jnp.zeros((TLON, CH), F32)
        for k, (a, b) in enumerate(TAPS):
            total += taps_ref[k : k + 1, :] * dep[r + 1 + a, 8 + b : 8 + b + TLON, :]
        send_grid[r] = total.astype(BF16)
        return carry

    lax.fori_loop(0, TLAT, grid_row, 0)
    for j in range(GRP - 1):
        remote(
            send_grid.at[lons[j]], grid_ref.at[lon], grid_send, grid_recv, lat, lons[j]
        ).start()
    mine_grid = pltpu.make_async_copy(send_grid.at[lon], grid_ref.at[lon], own_sem.at[0])
    mine_grid.start()


    for g in range(N_GRP):
        wait_got(parts.at[pl.ds(g * GRP, members(g))], part_recv.at[g])

    mine = jnp.sum(parts[...].astype(F32), axis=0).astype(BF16)
    red[...] = mine
    mine_share = pltpu.make_async_copy(red, shared.at[me], own_sem.at[1])
    mine_share.start()

    def send_share(g, j, to_lat, to_lon):
        remote(
            red, shared.at[me], share_send.at[g], share_recv.at[g], to_lat, to_lon
        ).start()


    each_peer(send_share)


    for g in range(N_GRP):
        wait_got(shared.at[pl.ds(g * GRP, members(g))], share_recv.at[g])

    mine_grid.wait()
    mine_share.wait()
    wait_got(grid_ref.at[pl.ds(0, GRP - 1)], grid_recv)
    for g in range(N_GRP):
        n = members(g)
        wait_sent(send_cells.at[g, pl.ds(0, n)], cell_send.at[g])
        wait_sent(send_rows.at[pl.ds(g * GRP, n)], row_send.at[g])
        wait_sent(chunks.at[pl.ds(g * GRP, n)], part_send.at[g])
        wait_sent(shared.at[pl.ds(g * GRP, n)], share_send.at[g])
    wait_sent(send_cot.at[pl.ds(0, GRP - 1)], cot_send)
    wait_sent(send_grid.at[pl.ds(0, GRP - 1)], grid_send)

    @pl.when(up_edge)
    def _():
        wait_sent(send_cot, edge_send.at[0])

    @pl.when(down_edge)
    def _():
        wait_sent(send_cot, edge_send.at[1])

    for i, (there, _, _, sr, sc, _, _) in enumerate(halos):
        def sent_halo(i=i, sr=sr, sc=sc):
            wait_sent(at(sr, sc), halo_send.at[i])

        sent_halo() if there is None else pl.when(there)(sent_halo)


def finish(
    grid_in, shared_in, grid_hbm, g_in_hbm, g_bias_hbm, g_out_hbm, g_taps_hbm,
    grid, shared, g_in, g_bias, g_out, g_taps, sem,
):
    come = pltpu.make_async_copy(shared_in, shared, sem.at[5])
    come.start()
    grid_come = pltpu.make_async_copy(grid_in, grid, sem.at[6])
    grid_come.start()
    copies = [pltpu.make_async_copy(grid, grid_hbm, sem.at[0])]
    come.wait()
    g_out[:, :128] = shared[32:64].astype(F32).reshape(HID, 128)
    g_out[:, 128:] = shared[64:96].astype(F32).reshape(HID, 128)
    copies.append(pltpu.make_async_copy(g_out, g_out_hbm, sem.at[1]))
    copies[1].start()
    g_in[...] = shared[0:32].astype(F32).reshape(HID, FEAT).T
    copies.append(pltpu.make_async_copy(g_in, g_in_hbm, sem.at[2]))
    copies[2].start()
    grid_come.wait()
    copies[0].start()
    small = (shared[96:99].astype(F32) + shared[99:102].astype(F32)).reshape(24, 128)
    for k in range(9):
        g_taps[k : k + 1, :128] = small[2 * k : 2 * k + 1]
        g_taps[k : k + 1, 128:] = small[2 * k + 1 : 2 * k + 2]
    g_bias[:, :128] = small[18:19]
    g_bias[:, 128:] = small[19:20]
    copies.append(pltpu.make_async_copy(g_taps, g_taps_hbm, sem.at[3]))
    copies.append(pltpu.make_async_copy(g_bias, g_bias_hbm, sem.at[4]))
    copies[3].start()
    copies[4].start()
    for copy in copies:
        copy.wait()


def local(obs, owner, cell, count, w_in, bias, w_out, taps, cot):
    hbm = pl.BlockSpec(memory_space=pltpu.HBM)
    dma = pltpu.SemaphoreType.DMA
    order = [dz * 32 + dc * 16 + dx * 4 + dy for dz, dc, dx, dy in PLACES]
    order = jnp.asarray(np.repeat(np.array(order, np.int32)[:, None], 128, axis=1))
    rows, shared = pl.pallas_call(
        kernel,
        name="encode_step",
        out_shape=(
            jax.ShapeDtypeStruct((GRP, TLON, CH), BF16),
            jax.ShapeDtypeStruct((N_DEV, 8, 128), BF16),
        ),
        in_specs=[hbm] * 10,
        out_specs=(hbm,) * 2,
        scratch_shapes=[
            pltpu.VMEM((OBS, FEAT), BF16),
            pltpu.VMEM((1, OBS), I32),
            pltpu.VMEM((OBS,), I32),
            pltpu.SMEM((1,), I32),
            pltpu.VMEM((N_DEV, 128), I32),
            pltpu.VMEM((FEAT, HID), BF16),
            pltpu.VMEM((1, HID), F32),
            pltpu.VMEM((HID, CH), BF16),
            pltpu.VMEM((9, CH), F32),
            pltpu.VMEM((GLON, CH), BF16),
            pltpu.VMEM((N_DEV, CAP, FEAT), BF16),
            pltpu.VMEM((N_DEV, CAP, FEAT), BF16),
            pltpu.VMEM((N_GRP, GRP, 128), F32),
            pltpu.VMEM((N_GRP, GRP, 128), F32),
            pltpu.VMEM((GRP, 26, CH), BF16),
            pltpu.VMEM((TLAT + 2, 26, CH), BF16),
            pltpu.VMEM((TLAT + 2, 40, CH), F32),
            pltpu.VMEM((3, TLAT + 2, TLON, CH), F32),
            pltpu.VMEM((TLAT + 2, 40, CH), F32),
            pltpu.VMEM((TLAT, TLON, CH), BF16),
            pltpu.VMEM((N_DEV, 8, 128), BF16),
            pltpu.VMEM((N_DEV, 8, 128), BF16),
            pltpu.VMEM((8, 128), BF16),
            pltpu.VMEM((HID, 2 * FEAT), F32),
            pltpu.VMEM((HID, CH), F32),
            pltpu.VMEM((CH, CELLS), BF16),
            pltpu.VMEM((CELLS, N_GRP * SLOTS), BF16),
            pltpu.VMEM((CH, N_GRP * SLOTS), BF16),
            pltpu.VMEM((HID, N_GRP * SLOTS), F32),
            dma((10,)), dma((2,)),
            dma((N_GRP,)), dma((N_GRP,)), dma((N_GRP,)), dma((N_GRP,)),
            dma, dma, dma((2,)), dma((2,)),
            dma((N_GRP,)), dma((N_GRP,)), dma((N_GRP,)), dma((N_GRP,)),
            dma((8,)), dma((8,)), dma, dma,
        ],
        compiler_params=pltpu.CompilerParams(
            collective_id=0, has_side_effects=True, vmem_limit_bytes=67043328
        ),
        cost_estimate=pl.CostEstimate(
            flops=4_000_000_000, bytes_accessed=2_000_000, transcendentals=800_000
        ),
    )(
        obs, owner.reshape(1, OBS), cell, count, order, w_in, bias.reshape(1, HID),
        w_out, taps, cot.reshape(GLON, CH),
    )
    outs = [((GRP, TLON, CH), BF16), ((FEAT, HID), F32), ((1, HID), F32), ((HID, CH), F32), ((9, CH), F32)]
    grid, g_in, g_bias, g_out, g_taps = pl.pallas_call(
        finish,
        name="finish",
        out_shape=tuple(jax.ShapeDtypeStruct(*o) for o in outs),
        in_specs=[hbm, hbm],
        out_specs=(hbm,) * 5,
        scratch_shapes=[
            pltpu.VMEM(*outs[0]),
            pltpu.VMEM((N_DEV, 8, 128), BF16),
            *[pltpu.VMEM(*o) for o in outs[1:]],
            dma((7,)),
        ],
        compiler_params=pltpu.CompilerParams(vmem_limit_bytes=67043328),
    )(rows, shared)
    return (grid.reshape(1, GLON, CH), g_in, g_bias.reshape(HID), g_out, g_taps)


def solution(mesh):
    block = P(("lat", "lon"))
    return jax.shard_map(
        local,
        mesh=mesh,
        in_specs=(block, block, block, block, P(), P(), P(), P(), block),
        out_specs=(block, P(), P(), P(), P()),
        check_vma=False,
    )
```
